32 devices in a mesh: rows: 8 (over z, y), rhs: 4 (over x, core).
Axes of the slice: x: 2, y: 2, z: 4, core: 2. Of those that a mesh axis runs over, the one named last changes fastest.
Arguments:
- right_sides: bfloat16 [64, 16384], P('rhs', 'rows'), may hold values from -6 to 6
- lower_inverse: bfloat16 [64, 256, 256], P('rows'), may hold values from -0.375 to 0.375
- lower_left: bfloat16 [64, 256, 32], P('rows'), may hold values from -1 to 1
- lower_right: bfloat16 [64, 256, 32], P('rows'), may hold values from -0.015625 to 0.015625
- upper_inverse: bfloat16 [64, 256, 256], P('rows'), may hold values from -0.375 to 0.375
- upper_left: bfloat16 [64, 256, 32], P('rows'), may hold values from -1 to 1
- upper_right: bfloat16 [64, 256, 32], P('rows'), may hold values from -0.015625 to 0.015625
- block_ranks: int32 [2, 64], P(None, 'rows'), may hold values from 8 to 32
Outputs:
- first_solve: float32 [64, 16384], P('rhs', 'rows')
- second_solve: float32 [64, 16384], P('rhs', 'rows')
The draws below stay inside these ranges and needn't reach their ends.
All inputs are finite; a program needn't handle non-finite values.
Results may differ from the reference program's by a relative error of at most 0.0051.
Values may be sent and summed in bfloat16 or wider, within the bound.
A program may use at most 64 MiB of HBM per device.

```python
import jax
import jax.numpy as jnp
from jax import lax

BS = 256
RANK = 32
RHS = 64
NBLK = 64
ORDER = 16384


def with_ends(drawn, own_key, low, largest):
    place = [jax.random.randint(jax.random.fold_in(own_key, axis), (), 0, length) for axis, length in enumerate(drawn.shape)]
    main_axis = drawn.shape.index(max(drawn.shape))
    beside = place[:main_axis] + [(place[main_axis] + 1) % drawn.shape[main_axis]] + place[main_axis + 1:]
    return drawn.at[tuple(place)].set(low).at[tuple(beside)].set(largest)


def levels(rng, extent, shards, least, high):
    gain = 1.0
    for position, shards_of in shards:
        heights = jax.random.uniform(jax.random.fold_in(jax.random.fold_in(rng, 6), position), (shards_of,), jnp.float32, least / len(shards), high / len(shards))
        gain = gain * jnp.repeat(jnp.exp(heights), extent[position] // shards_of).reshape((-1,) + (1,) * (len(extent) - 1 - position))
    return gain


def bell_draw(own_key, shape, deviation, bound, pieces=(), kind=jnp.bfloat16):
    entries = jax.random.normal(own_key, shape, jnp.float32) * deviation
    if len(pieces) > 0:
        entries = levels(own_key, shape, pieces, -0.22, 0.18) * entries
    return jnp.clip(entries, min=-bound, max=bound).astype(kind)


def setup_inputs(seed: int = 0) -> dict:
    arg_keys = jax.random.split(jax.random.key(seed), 9)
    right_sides = bell_draw(arg_keys[0], (RHS, ORDER), 1.0, 6.0, ((0, 4), (1, 8)))
    lower_inverse = bell_draw(arg_keys[1], (NBLK, BS, BS), BS ** -0.5, 0.375, ((0, 8),))
    lower_left = bell_draw(arg_keys[2], (NBLK, BS, RANK), RANK ** -0.5, 1.0, ((0, 8),))
    lower_right = bell_draw(arg_keys[3], (NBLK, BS, RANK), (8 * NBLK * BS) ** -0.5, 0.015625, ((0, 8),))
    upper_inverse = bell_draw(arg_keys[4], (NBLK, BS, BS), BS ** -0.5, 0.375, ((0, 8),))
    upper_left = bell_draw(arg_keys[5], (NBLK, BS, RANK), RANK ** -0.5, 1.0, ((0, 8),))
    upper_right = bell_draw(arg_keys[6], (NBLK, BS, RANK), (8 * NBLK * BS) ** -0.5, 0.015625, ((0, 8),))
    block_ranks = with_ends(jax.random.randint(arg_keys[7], (2, NBLK), RANK // 4, RANK + 1), jax.random.fold_in(arg_keys[7], 1), RANK // 4, RANK).astype(jnp.int32)
    return {"right_sides": right_sides, "lower_inverse": lower_inverse, "lower_left": lower_left, "lower_right": lower_right, "upper_inverse": upper_inverse, "upper_left": upper_left, "upper_right": upper_right, "block_ranks": block_ranks}


highest = lax.Precision.HIGHEST


def factors(inverse, left_factor, right_factor, ranks_row):
    product = jnp.einsum("bij,bjk->bik", inverse.astype(jnp.float32), left_factor.astype(jnp.float32))
    rounded = lax.optimization_barrier(product.astype(jnp.bfloat16))
    coupled = rounded.astype(jnp.float32)
    columns = jnp.arange(RANK, dtype=jnp.int32)
    rank_mask = (columns[None, :] < ranks_row[:, None]).astype(jnp.float32)
    masked = right_factor.astype(jnp.float32) * rank_mask[:, None, :]
    return coupled, masked


def sweep_blocks(values, inverse, coupled, masked, reverse):
    blocked = values.reshape(RHS, NBLK, BS).astype(jnp.float32)
    pushed = jnp.einsum("rbk,bjk->brj", blocked, inverse.astype(jnp.float32))

    def advance(state, inputs):
        pushed_row, coupled_row, masked_row = inputs
        solved = pushed_row - jnp.dot(state, coupled_row.T, precision=highest)
        state = state + jnp.dot(solved, masked_row, precision=highest)
        return state, solved

    start = jnp.zeros((RHS, RANK), jnp.float32)
    _, solved = lax.scan(advance, start, (pushed, coupled, masked), reverse=reverse)
    return jnp.transpose(solved, (1, 0, 2)).reshape(RHS, NBLK * BS)


def reference(right_sides, lower_inverse, lower_left, lower_right, upper_inverse, upper_left, upper_right, block_ranks):
    lower_coupled, lower_masked = factors(lower_inverse, lower_left, lower_right, block_ranks[0])
    upper_coupled, upper_masked = factors(upper_inverse, upper_left, upper_right, block_ranks[1])
    forward = sweep_blocks(right_sides, lower_inverse, lower_coupled, lower_masked, False)
    first_solve = sweep_blocks(forward.astype(jnp.bfloat16), upper_inverse, upper_coupled, upper_masked, True)
    forward_again = sweep_blocks(first_solve.astype(jnp.bfloat16), lower_inverse, lower_coupled, lower_masked, False)
    second_solve = sweep_blocks(forward_again.astype(jnp.bfloat16), upper_inverse, upper_coupled, upper_masked, True)
    return first_solve, second_solve
```

```python
import functools

import jax
import jax.numpy as jnp
from jax import lax
from jax.experimental import pallas as pl
from jax.experimental.pallas import tpu as pltpu
from jax.sharding import PartitionSpec as P

MESH = pl.DeviceIdType.MESH
LANES = 128
f32, bf16 = jnp.float32, jnp.bfloat16


def split(x):
    hi = x.astype(bf16)
    return hi, (x - hi.astype(f32)).astype(bf16)


def dot(a, b):
    return jnp.dot(a, b, preferred_element_type=f32)


def dot_nt(a, b):
    return lax.dot_general(a, b, (((1,), (1,)), ((), ())), preferred_element_type=f32)


def dot_split(a, b_hi, b_lo):
    a_hi, a_lo = split(a)
    rows = a.shape[0]
    both = dot(jnp.concatenate([a_hi, a_lo], axis=0), b_hi)
    return both[:rows] + both[rows:] + dot(a_hi, b_lo)


def dot_full(a, b):
    return dot_split(a, *split(b))


def grow(x, rows):
    if x.shape[0] == rows:
        return x
    return jnp.concatenate([x, jnp.zeros((rows - x.shape[0], LANES), f32)], axis=0)


def each(count, body):
    if count <= 8:
        for i in range(count):
            body(i)
    else:
        lax.fori_loop(0, count, lambda i, c: (body(i), c)[1], 0)


def kernel(
    R, nb, bs, w, n,
    rhs_h, linv_h, llt_h, lrt_h, uinv_h, ult_h, urt_h, ranks_h,
    first, second,
    rhs, llt, lrt, ult, urt, ranks,
    inv, ctp, ntp, wst, hs, got0, got1, got2, send0, send1, send2, g, walk, table, y,
    load_sem, block_sem, send_sem, recv_sem,
):
    me = lax.axis_index("rows")
    group = LANES // w
    quads = nb // group
    half = n // 2

    small = [
        pltpu.make_async_copy(src, dst, load_sem.at[i])
        for i, (src, dst) in enumerate(
            ((llt_h, llt), (lrt_h, lrt), (ranks_h, ranks), (ult_h, ult), (urt_h, urt), (rhs_h, rhs))
        )
    ]
    large = [
        [
            pltpu.make_async_copy(src.at[b], inv.at[f, b], block_sem.at[f, b])
            for b in (range(nb) if f == 0 else reversed(range(nb)))
        ]
        for f, src in ((0, linv_h), (1, uinv_h))
    ]
    for cp in small[:3] + large[0] + small[3:5] + large[1] + small[5:]:
        cp.start()

    barrier = pltpu.get_barrier_semaphore()

    def greet(i):
        pl.semaphore_signal(
            barrier, inc=1, device_id={"rows": lax.rem(me + i + 1, R)}, device_id_type=MESH
        )

    each(R - 1, greet)

    ctp[...] = jnp.zeros_like(ctp)
    ntp[...] = jnp.zeros_like(ntp)

    lane = lax.broadcasted_iota(jnp.int32, (w, LANES), 1)
    row = lax.broadcasted_iota(jnp.int32, (w, LANES), 0)
    eye = (lax.rem(lane, w) == row).astype(f32)

    def lanes(rows):
        return lax.broadcasted_iota(jnp.int32, (rows, LANES), 1)

    def block(f, p):
        return p if f == 0 else nb - 1 - p

    lefts, rights = (llt, ult), (lrt, urt)
    kernels = ([], [])
    maps = [None, None]
    for f in (0, 1):
        for cp in small[:3] if f == 0 else small[3:5]:
            cp.wait()
        wide_row = lax.broadcasted_iota(jnp.int32, (w, bs), 0)
        for p in range(nb):
            b = block(f, p)
            large[f][p].wait()
            at = pl.ds(w * (p % group), w)
            ct = dot_nt(lefts[f][b], inv[f, b]).astype(bf16)
            ctp[f, p, at, :] = ct
            mt = jnp.where(wide_row < ranks[f, b], rights[f][b].astype(f32), 0.0).astype(bf16)
            hi, lo = split(dot(mt, inv[f, b]))
            ntp[f, 0, p, at, :] = hi
            ntp[f, 1, p, at, :] = lo
            kernels[f].append(eye - dot_nt(ct, jnp.concatenate([mt] * group, axis=0)))

    chains = {}
    for q in range(quads):
        for f in (0, 1):
            chains[f, q] = [eye]
    for k in range(group):
        for q in range(quads):
            for f in (0, 1):
                last = chains[f, q][-1]
                moved = dot_full(last[:, :w], kernels[f][q * group + k])
                chains[f, q].append(jnp.concatenate([moved, eye], axis=0))

    full = w * (nb + 1)
    joined = {}
    for f in (0, 1):
        before = None
        for q in range(quads):
            grown = w * (group + 1)
            total = jnp.zeros((grown, LANES), f32)
            for k in range(group):
                col = chains[f, q][k]
                total = jnp.where(lanes(grown) // w == k, grow(col, grown), total)
            end = chains[f, q][group]
            if before is not None:
                moved = dot_full(before[:, :w], jnp.concatenate([total[:w], end[:w]], axis=1))
                total = jnp.concatenate([moved[:, :LANES], total[w:]], axis=0)
                end = jnp.concatenate([moved[:, LANES:], end[w:]], axis=0)
            joined[f, q] = grow(total, full)
            before = end
        maps[f] = before[:w]
        hi, lo = split(before[w:])
        wst[f, 0, quads] = hi
        wst[f, 1, quads] = lo

    narrow = w // group
    narrow_lanes = lanes(narrow) // w

    def fold_map(x):
        out = x[:narrow]
        for k in range(1, group):
            out = jnp.where(narrow_lanes == k, x[k * narrow : (k + 1) * narrow], out)
        return out

    def tile(x):
        return jnp.concatenate([x] * group, axis=0)

    def expand(x):
        return jnp.where(lane // w == row // narrow, tile(x), 0.0)

    def copy(k, src, dst, i):
        peer = lax.rem(me + i + 1, R)
        return pltpu.make_async_remote_copy(
            src_ref=src, dst_ref=dst.at[me], send_sem=send_sem.at[k, i],
            recv_sem=recv_sem.at[k, me], device_id={"rows": peer}, device_id_type=MESH,
        )

    def arrive(k, src, dst, i):
        peer = lax.rem(me + i + 1, R)
        pltpu.make_async_remote_copy(
            src_ref=src, dst_ref=dst.at[peer], send_sem=send_sem.at[k, i],
            recv_sem=recv_sem.at[k, peer], device_id={"rows": peer}, device_id_type=MESH,
        ).wait_recv()

    send0[:narrow] = fold_map(maps[0])
    send0[narrow:] = fold_map(maps[1])
    pl.semaphore_wait(barrier, R - 1)
    each(R - 1, lambda i: copy(0, send0, got0, i).start())
    got0[me] = send0[...]

    for f in (0, 1):
        for q in range(quads):
            total = joined[f, q]
            hi, lo = split(total[w:])
            wst[f, 0, q] = hi
            wst[f, 1, q] = lo
            p_hi, p_lo = split(total[:w])
            lhs = jnp.concatenate([p_hi, p_lo], axis=0)
            for k in range(group):
                p = q * group + k
                b = block(f, p)
                both = dot(lhs, ctp[f, p])
                hi, lo = split(both[:w] + both[w:])
                hs[f, :, b * bs : (b + 1) * bs] = jnp.concatenate([hi, hi, lo, lo], axis=0)

    def pushes(f, piece):
        parts = []
        for q in range(quads):
            total = None
            for k in range(group):
                p = q * group + k
                v = piece(block(f, p))
                term = dot_nt(v, ntp[f, 0, p]) + dot_nt(v, ntp[f, 1, p])
                total = term if total is None else total + term
            parts.append(total)
        return jnp.concatenate(parts, axis=1)

    def message(f, u):
        return dot_split(u, wst[f, 0, quads], wst[f, 1, quads])

    def local_blocks(f, piece, u):
        out = {}
        for q in range(quads):
            x_hi, x_lo = split(dot_split(u, wst[f, 0, q], wst[f, 1, q]))
            lhs = jnp.concatenate([x_hi, x_lo], axis=0)
            for k in range(group):
                p = q * group + k
                b = block(f, p)
                both = dot(lhs, ctp[f, p])
                out[b] = dot_nt(piece(b), inv[f, b]) - both[:n] - both[n:]
        return out

    def cols(b):
        return slice(b * bs, (b + 1) * bs)

    def fold(m, z):
        mixed = jnp.where(lax.rem(lanes(n) // w, 2) == 0, m, z)
        return jnp.where(lanes(half) < LANES // 2, mixed[:half], mixed[half:])

    def unfold(x):
        low = lanes(half) < LANES // 2
        return jnp.concatenate([jnp.where(low, x, 0.0), jnp.where(low, 0.0, x)], axis=0)

    def sweep_start(piece):
        u = pushes(0, piece)
        m = message(0, u)
        out = local_blocks(0, piece, u)
        for b in range(nb):
            y[:, cols(b)] = out[b]
        return m

    def incoming(arrived):
        a = jnp.concatenate([unfold(arrived(e)) for e in range(R)], axis=1)
        a_hi, a_lo = split(a)
        both = jnp.concatenate([a_hi, a_lo], axis=0)
        states = []
        for k in (0, 1):
            r = dot(both, table[k, 0])
            s_hi, s_lo = split(r[:n] + r[n:] + dot(a_hi, table[k, 1]))
            even = lax.rem(lanes(n) // w, 2) == 0
            states.append(jnp.where(even, s_hi.astype(f32), s_lo.astype(f32)).astype(bf16))
        return states

    def sweep_end(s_f, s_b, out_ref):
        forward = [
            (y[:, cols(b)] - dot(s_f, hs[0, :, cols(b)])).astype(bf16) for b in range(nb)
        ]
        piece = lambda b: forward[b]
        u = pushes(1, piece)
        out = local_blocks(1, piece, u)
        for b in range(nb):
            out_ref[:, cols(b)] = out[b] - dot(s_b, hs[1, :, cols(b)])

    small[5].wait()
    m = sweep_start(lambda b: rhs[:, cols(b)])
    mixed = pushes(
        1,
        lambda b: jnp.concatenate(
            [*split(y[:, cols(b)]), hs[0, :w, cols(b)], hs[0, 2 * w : 3 * w, cols(b)]], axis=0
        ),
    )
    u = jnp.concatenate(
        [mixed[:n] + mixed[n : 2 * n], mixed[2 * n : 2 * n + w] + mixed[2 * n + w :]], axis=0
    )
    zm = message(1, u)
    send1[:narrow] = fold_map(zm[n:])
    send1[narrow:] = fold(m, zm[:n])
    each(R - 1, lambda i: copy(1, send1, got1, i).start())
    got1[me] = send1[...]

    zero = jnp.zeros((w, LANES), f32)
    spot = jnp.where(lane < w, eye, 0.0)
    each(R - 1, lambda i: arrive(0, send0, got0, i))
    g[1, 0:w] = zero

    def rows_of(d):
        return pl.ds(d * w if isinstance(d, int) else pl.multiple_of(d * w, w), w)

    def backward_map(d):
        moved = dot_full(expand(got0[d, narrow:]), tile(g[1, rows_of(d)]))
        g[1, rows_of(d + 1)] = moved + jnp.where(me == d, eye, 0.0)

    def forward_map(d, state):
        return dot_full(state, tile(expand(got0[d, :narrow])))

    def crossed(d, state):
        return dot_full(
            dot_full(state, tile(expand(got1[d, :narrow]))), tile(g[1, rows_of(d)])
        )

    if R <= 8:
        history = [None]
        for d in range(R - 1):
            backward_map(d)
            last = history[-1]
            grown = spot if last is None else jnp.concatenate([forward_map(d, last), spot], axis=0)
            history.append(grown)
        chosen = jnp.zeros((R * w, LANES), f32)
        for d in range(1, R):
            chosen = jnp.where(me == d, grow(history[d], R * w), chosen)
        g[0] = chosen
        each(R - 1, lambda i: arrive(1, send1, got1, i))
        total = jnp.zeros((R * w, LANES), f32)
        for d in range(1, R):
            total += grow(crossed(d, history[d]), R * w)
        g[2] = total
    else:
        each(R - 1, backward_map)
        each(R - 1, lambda i: arrive(1, send1, got1, i))
        walk[...] = jnp.zeros_like(walk)
        g[0] = jnp.zeros((R * w, LANES), f32)
        g[2] = jnp.zeros((R * w, LANES), f32)

        def step(d):
            state = walk[...]
            g[0] = jnp.where(me == d, state, g[0])
            g[2] = g[2] + crossed(d, state)
            walk[...] = forward_map(d, state)
            walk[rows_of(d)] = spot

        each(R, step)

    c_hi, c_lo = split(g[0])
    spread = tile(eye).astype(bf16)
    g[0] = dot(c_hi, spread) + dot(c_lo, spread)

    def fill(e):
        at = pl.ds(e * LANES if isinstance(e, int) else pl.multiple_of(e * LANES, LANES), LANES)
        hi, lo = split(jnp.concatenate([g[0, rows_of(e)], zero] * 2, axis=0))
        table[0, 0, at] = hi
        table[0, 1, at] = lo
        hi, lo = split(jnp.concatenate([-g[2, rows_of(e)], g[1, rows_of(e)]] * 2, axis=0))
        table[1, 0, at] = hi
        table[1, 1, at] = lo

    each(R, fill)

    s_f, s_b = incoming(lambda e: got1[e, narrow:])
    sweep_end(s_f, s_b, first)

    m = sweep_start(lambda b: first[:, cols(b)].astype(bf16))
    mixed = pushes(1, lambda b: jnp.concatenate(split(y[:, cols(b)]), axis=0))
    z = message(1, mixed[:n] + mixed[n:])
    send2[...] = fold(m, z)
    each(R - 1, lambda i: copy(2, send2, got2, i).start())
    got2[me] = send2[...]
    each(R - 1, lambda i: arrive(2, send2, got2, i))
    s_f, s_b = incoming(lambda e: got2[e])
    sweep_end(s_f, s_b, second)

    each(R - 1, lambda i: copy(0, send0, got0, i).wait_send())
    each(R - 1, lambda i: copy(1, send1, got1, i).wait_send())
    each(R - 1, lambda i: copy(2, send2, got2, i).wait_send())


def local(R, rhs, linv, lleft, lright, uinv, uleft, uright, ranks):
    nb, bs, w = lleft.shape
    n = rhs.shape[0]
    flip = lambda a: jnp.swapaxes(a, 1, 2)
    vmem = pl.BlockSpec(memory_space=pltpu.VMEM)
    hbm = pl.BlockSpec(memory_space=pltpu.HBM)
    quads = nb * w // LANES
    out = jax.ShapeDtypeStruct(rhs.shape, f32)
    narrow = w * w // LANES
    packed = narrow + n // 2
    slim = pltpu.VMEM((nb, w, bs), bf16)
    return pl.pallas_call(
        functools.partial(kernel, R, nb, bs, w, n),
        out_shape=(out, out),
        in_specs=[hbm] * 8,
        out_specs=(vmem, vmem),
        scratch_shapes=[
            pltpu.VMEM(rhs.shape, bf16),
            slim, slim, slim, slim,
            pltpu.SMEM(ranks.shape, jnp.int32),
            pltpu.VMEM((2, nb, bs, bs), bf16),
            pltpu.VMEM((2, nb, LANES, bs), bf16),
            pltpu.VMEM((2, 2, nb, LANES, bs), bf16),
            pltpu.VMEM((2, 2, quads + 1, nb * w, LANES), bf16),
            pltpu.VMEM((2, 4 * w, nb * bs), bf16),
            pltpu.VMEM((R, 2 * narrow, LANES), f32),
            pltpu.VMEM((R, packed, LANES), f32),
            pltpu.VMEM((R, n // 2, LANES), f32),
            pltpu.VMEM((2 * narrow, LANES), f32),
            pltpu.VMEM((packed, LANES), f32),
            pltpu.VMEM((n // 2, LANES), f32),
            pltpu.VMEM((3, R * w, LANES), f32),
            pltpu.VMEM((R * w, LANES), f32),
            pltpu.VMEM((2, 2, R * LANES, LANES), bf16),
            pltpu.VMEM((n, nb * bs), f32),
            pltpu.SemaphoreType.DMA((6,)),
            pltpu.SemaphoreType.DMA((2, nb)),
            pltpu.SemaphoreType.DMA((3, R)),
            pltpu.SemaphoreType.DMA((3, R)),
        ],
        compiler_params=pltpu.CompilerParams(
            collective_id=0, has_side_effects=True, vmem_limit_bytes=33554432
        ),
    )(rhs, linv, flip(lleft), flip(lright), uinv, flip(uleft), flip(uright), ranks)


def solution(mesh):
    blocks = P("rows", None, None)
    placed = (P("rhs", "rows"),) + (blocks,) * 6 + (P(None, "rows"),)
    return jax.shard_map(
        functools.partial(local, mesh.shape["rows"]),
        mesh=mesh,
        in_specs=placed,
        out_specs=(P("rhs", "rows"), P("rhs", "rows")),
        check_vma=False,
    )
```

```python
import functools

import jax
import jax.numpy as jnp
from jax import lax
from jax.experimental import pallas as pl
from jax.experimental.pallas import tpu as pltpu
from jax.sharding import PartitionSpec as P

MESH = pl.DeviceIdType.MESH
LANES = 128
f32, bf16 = jnp.float32, jnp.bfloat16


def split(x):
    hi = x.astype(bf16)
    return hi, (x - hi.astype(f32)).astype(bf16)


def dot(a, b):
    return jnp.dot(a, b, preferred_element_type=f32)


def dot_nt(a, b):
    return lax.dot_general(a, b, (((1,), (1,)), ((), ())), preferred_element_type=f32)


def dot_split(a, b_hi, b_lo):
    a_hi, a_lo = split(a)
    rows = a.shape[0]
    both = dot(jnp.concatenate([a_hi, a_lo], axis=0), b_hi)
    return both[:rows] + both[rows:] + dot(a_hi, b_lo)


def dot_full(a, b):
    return dot_split(a, *split(b))


def grow(x, rows):
    if x.shape[0] == rows:
        return x
    return jnp.concatenate([x, jnp.zeros((rows - x.shape[0], LANES), f32)], axis=0)


def each(count, body):
    if count <= 8:
        for i in range(count):
            body(i)
    else:
        lax.fori_loop(0, count, lambda i, c: (body(i), c)[1], 0)


def kernel(
    R, nb, bs, w, n,
    rhs_h, linv_h, llt_h, lrt_h, uinv_h, ult_h, urt_h, ranks_h,
    first, second,
    rhs, llt, lrt, ult, urt, ranks,
    inv, ctp, ntp, wst, hs, got0, got1, got2, send0, send1, send2, g, walk, table, y,
    load_sem, block_sem, send_sem, recv_sem,
):
    me = lax.axis_index("rows")
    group = LANES // w
    quads = nb // group
    half = n // 2

    small = [
        pltpu.make_async_copy(src, dst, load_sem.at[i])
        for i, (src, dst) in enumerate(
            ((llt_h, llt), (lrt_h, lrt), (ranks_h, ranks), (ult_h, ult), (urt_h, urt), (rhs_h, rhs))
        )
    ]
    large = [
        [
            pltpu.make_async_copy(src.at[b], inv.at[f, b], block_sem.at[f, b])
            for b in (range(nb) if f == 0 else reversed(range(nb)))
        ]
        for f, src in ((0, linv_h), (1, uinv_h))
    ]
    for cp in small[:3] + large[0] + small[3:5] + large[1] + small[5:]:
        cp.start()

    barrier = pltpu.get_barrier_semaphore()

    def greet(i):
        pl.semaphore_signal(
            barrier, inc=1, device_id={"rows": lax.rem(me + i + 1, R)}, device_id_type=MESH
        )

    each(R - 1, greet)

    ctp[...] = jnp.zeros_like(ctp)
    ntp[...] = jnp.zeros_like(ntp)

    lane = lax.broadcasted_iota(jnp.int32, (w, LANES), 1)
    row = lax.broadcasted_iota(jnp.int32, (w, LANES), 0)
    eye = (lax.rem(lane, w) == row).astype(f32)

    def lanes(rows):
        return lax.broadcasted_iota(jnp.int32, (rows, LANES), 1)

    def block(f, p):
        return p if f == 0 else nb - 1 - p

    lefts, rights = (llt, ult), (lrt, urt)
    kernels = ([], [])
    maps = [None, None]
    for f in (0, 1):
        for cp in small[:3] if f == 0 else small[3:5]:
            cp.wait()
        wide_row = lax.broadcasted_iota(jnp.int32, (w, bs), 0)
        for p in range(nb):
            b = block(f, p)
            large[f][p].wait()
            at = pl.ds(w * (p % group), w)
            ct = dot_nt(lefts[f][b], inv[f, b]).astype(bf16)
            ctp[f, p, at, :] = ct
            mt = jnp.where(wide_row < ranks[f, b], rights[f][b].astype(f32), 0.0).astype(bf16)
            hi, lo = split(dot(mt, inv[f, b]))
            ntp[f, 0, p, at, :] = hi
            ntp[f, 1, p, at, :] = lo
            kernels[f].append(eye - dot_nt(ct, jnp.concatenate([mt] * group, axis=0)))

    chains = {}
    for q in range(quads):
        for f in (0, 1):
            chains[f, q] = [eye]
    for k in range(group):
        for q in range(quads):
            for f in (0, 1):
                last = chains[f, q][-1]
                moved = dot_full(last[:, :w], kernels[f][q * group + k])
                chains[f, q].append(jnp.concatenate([moved, eye], axis=0))

    full = w * (nb + 1)
    joined = {}
    for f in (0, 1):
        before = None
        for q in range(quads):
            grown = w * (group + 1)
            total = jnp.zeros((grown, LANES), f32)
            for k in range(group):
                col = chains[f, q][k]
                total = jnp.where(lanes(grown) // w == k, grow(col, grown), total)
            end = chains[f, q][group]
            if before is not None:
                moved = dot_full(before[:, :w], jnp.concatenate([total[:w], end[:w]], axis=1))
                total = jnp.concatenate([moved[:, :LANES], total[w:]], axis=0)
                end = jnp.concatenate([moved[:, LANES:], end[w:]], axis=0)
            joined[f, q] = grow(total, full)
            before = end
        maps[f] = before[:w]
        hi, lo = split(before[w:])
        wst[f, 0, quads] = hi
        wst[f, 1, quads] = lo

    narrow = w // group
    narrow_lanes = lanes(narrow) // w

    def fold_map(x):
        out = x[:narrow]
        for k in range(1, group):
            out = jnp.where(narrow_lanes == k, x[k * narrow : (k + 1) * narrow], out)
        return out

    def tile(x):
        return jnp.concatenate([x] * group, axis=0)

    def expand(x):
        return jnp.where(lane // w == row // narrow, tile(x), 0.0)

    def copy(k, src, dst, i):
        peer = lax.rem(me + i + 1, R)
        return pltpu.make_async_remote_copy(
            src_ref=src, dst_ref=dst.at[me], send_sem=send_sem.at[k, i],
            recv_sem=recv_sem.at[k, me], device_id={"rows": peer}, device_id_type=MESH,
        )

    def arrive(k, src, dst, i):
        peer = lax.rem(me + i + 1, R)
        pltpu.make_async_remote_copy(
            src_ref=src, dst_ref=dst.at[peer], send_sem=send_sem.at[k, i],
            recv_sem=recv_sem.at[k, peer], device_id={"rows": peer}, device_id_type=MESH,
        ).wait_recv()

    send0[:narrow] = fold_map(maps[0])
    send0[narrow:] = fold_map(maps[1])
    pl.semaphore_wait(barrier, R - 1)
    each(R - 1, lambda i: copy(0, send0, got0, i).start())
    got0[me] = send0[...]

    for f in (0, 1):
        for q in range(quads):
            total = joined[f, q]
            hi, lo = split(total[w:])
            wst[f, 0, q] = hi
            wst[f, 1, q] = lo
            p_hi, p_lo = split(total[:w])
            lhs = jnp.concatenate([p_hi, p_lo], axis=0)
            for k in range(group):
                p = q * group + k
                b = block(f, p)
                both = dot(lhs, ctp[f, p])
                hi, lo = split(both[:w] + both[w:])
                hs[f, :, b * bs : (b + 1) * bs] = jnp.concatenate([hi, hi, lo, lo], axis=0)

    def pushes(f, piece):
        parts = []
        for q in range(quads):
            total = None
            for k in range(group):
                p = q * group + k
                v = piece(block(f, p))
                term = dot_nt(v, ntp[f, 0, p]) + dot_nt(v, ntp[f, 1, p])
                total = term if total is None else total + term
            parts.append(total)
        return jnp.concatenate(parts, axis=1)

    def message(f, u):
        return dot_split(u, wst[f, 0, quads], wst[f, 1, quads])

    def local_blocks(f, piece, u):
        out = {}
        for q in range(quads):
            x_hi, x_lo = split(dot_split(u, wst[f, 0, q], wst[f, 1, q]))
            lhs = jnp.concatenate([x_hi, x_lo], axis=0)
            for k in range(group):
                p = q * group + k
                b = block(f, p)
                both = dot(lhs, ctp[f, p])
                out[b] = dot_nt(piece(b), inv[f, b]) - both[:n] - both[n:]
        return out

    def cols(b):
        return slice(b * bs, (b + 1) * bs)

    def fold(m, z):
        mixed = jnp.where(lax.rem(lanes(n) // w, 2) == 0, m, z)
        return jnp.where(lanes(half) < LANES // 2, mixed[:half], mixed[half:])

    def unfold(x):
        low = lanes(half) < LANES // 2
        return jnp.concatenate([jnp.where(low, x, 0.0), jnp.where(low, 0.0, x)], axis=0)

    def sweep_start(piece):
        u = pushes(0, piece)
        m = message(0, u)
        out = local_blocks(0, piece, u)
        for b in range(nb):
            y[:, cols(b)] = out[b]
        return m

    def incoming(arrived):
        a = jnp.concatenate([unfold(arrived(e)) for e in range(R)], axis=1)
        a_hi, a_lo = split(a)
        both = jnp.concatenate([a_hi, a_lo], axis=0)
        states = []
        for k in (0, 1):
            r = dot(both, table[k, 0])
            s_hi, s_lo = split(r[:n] + r[n:] + dot(a_hi, table[k, 1]))
            even = lax.rem(lanes(n) // w, 2) == 0
            states.append(jnp.where(even, s_hi.astype(f32), s_lo.astype(f32)).astype(bf16))
        return states

    def sweep_end(s_f, s_b, out_ref):
        forward = [
            (y[:, cols(b)] - dot(s_f, hs[0, :, cols(b)])).astype(bf16) for b in range(nb)
        ]
        piece = lambda b: forward[b]
        u = pushes(1, piece)
        out = local_blocks(1, piece, u)
        for b in range(nb):
            out_ref[:, cols(b)] = out[b] - dot(s_b, hs[1, :, cols(b)])

    small[5].wait()
    m = sweep_start(lambda b: rhs[:, cols(b)])
    mixed = pushes(
        1,
        lambda b: jnp.concatenate(
            [*split(y[:, cols(b)]), hs[0, :w, cols(b)], hs[0, 2 * w : 3 * w, cols(b)]], axis=0
        ),
    )
    u = jnp.concatenate(
        [mixed[:n] + mixed[n : 2 * n], mixed[2 * n : 2 * n + w] + mixed[2 * n + w :]], axis=0
    )
    zm = message(1, u)
    send1[:narrow] = fold_map(zm[n:])
    send1[narrow:] = fold(m, zm[:n])
    each(R - 1, lambda i: copy(1, send1, got1, i).start())
    got1[me] = send1[...]

    zero = jnp.zeros((w, LANES), f32)
    spot = jnp.where(lane < w, eye, 0.0)
    each(R - 1, lambda i: arrive(0, send0, got0, i))
    g[1, 0:w] = zero

    def rows_of(d):
        return pl.ds(d * w if isinstance(d, int) else pl.multiple_of(d * w, w), w)

    def backward_map(d):
        moved = dot_full(expand(got0[d, narrow:]), tile(g[1, rows_of(d)]))
        g[1, rows_of(d + 1)] = moved + jnp.where(me == d, eye, 0.0)

    def forward_map(d, state):
        return dot_full(state, tile(expand(got0[d, :narrow])))

    def crossed(d, state):
        return dot_full(
            dot_full(state, tile(expand(got1[d, :narrow]))), tile(g[1, rows_of(d)])
        )

    if R <= 8:
        history = [None]
        for d in range(R - 1):
            backward_map(d)
            last = history[-1]
            grown = spot if last is None else jnp.concatenate([forward_map(d, last), spot], axis=0)
            history.append(grown)
        chosen = jnp.zeros((R * w, LANES), f32)
        for d in range(1, R):
            chosen = jnp.where(me == d, grow(history[d], R * w), chosen)
        g[0] = chosen
        each(R - 1, lambda i: arrive(1, send1, got1, i))
        total = jnp.zeros((R * w, LANES), f32)
        for d in range(1, R):
            total += grow(crossed(d, history[d]), R * w)
        g[2] = total
    else:
        each(R - 1, backward_map)
        each(R - 1, lambda i: arrive(1, send1, got1, i))
        walk[...] = jnp.zeros_like(walk)
        g[0] = jnp.zeros((R * w, LANES), f32)
        g[2] = jnp.zeros((R * w, LANES), f32)

        def step(d):
            state = walk[...]
            g[0] = jnp.where(me == d, state, g[0])
            g[2] = g[2] + crossed(d, state)
            walk[...] = forward_map(d, state)
            walk[rows_of(d)] = spot

        each(R, step)

    c_hi, c_lo = split(g[0])
    spread = tile(eye).astype(bf16)
    g[0] = dot(c_hi, spread) + dot(c_lo, spread)

    def fill(e):
        at = pl.ds(e * LANES if isinstance(e, int) else pl.multiple_of(e * LANES, LANES), LANES)
        hi, lo = split(jnp.concatenate([g[0, rows_of(e)], zero] * 2, axis=0))
        table[0, 0, at] = hi
        table[0, 1, at] = lo
        hi, lo = split(jnp.concatenate([-g[2, rows_of(e)], g[1, rows_of(e)]] * 2, axis=0))
        table[1, 0, at] = hi
        table[1, 1, at] = lo

    each(R, fill)

    s_f, s_b = incoming(lambda e: got1[e, narrow:])
    sweep_end(s_f, s_b, first)

    m = sweep_start(lambda b: first[:, cols(b)].astype(bf16))
    mixed = pushes(1, lambda b: jnp.concatenate(split(y[:, cols(b)]), axis=0))
    z = message(1, mixed[:n] + mixed[n:])
    send2[...] = fold(m, z)
    each(R - 1, lambda i: copy(2, send2, got2, i).start())
    got2[me] = send2[...]
    each(R - 1, lambda i: arrive(2, send2, got2, i))
    s_f, s_b = incoming(lambda e: got2[e])
    sweep_end(s_f, s_b, second)

    each(R - 1, lambda i: copy(0, send0, got0, i).wait_send())
    each(R - 1, lambda i: copy(1, send1, got1, i).wait_send())
    each(R - 1, lambda i: copy(2, send2, got2, i).wait_send())


def local(R, rhs, linv, lleft, lright, uinv, uleft, uright, ranks):
    nb, bs, w = lleft.shape
    n = rhs.shape[0]
    flip = lambda a: jnp.swapaxes(a, 1, 2)
    vmem = pl.BlockSpec(memory_space=pltpu.VMEM)
    hbm = pl.BlockSpec(memory_space=pltpu.HBM)
    quads = nb * w // LANES
    out = jax.ShapeDtypeStruct(rhs.shape, f32)
    narrow = w * w // LANES
    packed = narrow + n // 2
    slim = pltpu.VMEM((nb, w, bs), bf16)
    return pl.pallas_call(
        functools.partial(kernel, R, nb, bs, w, n),
        out_shape=(out, out),
        in_specs=[hbm] * 8,
        out_specs=(vmem, vmem),
        scratch_shapes=[
            pltpu.VMEM(rhs.shape, bf16),
            slim, slim, slim, slim,
            pltpu.SMEM(ranks.shape, jnp.int32),
            pltpu.VMEM((2, nb, bs, bs), bf16),
            pltpu.VMEM((2, nb, LANES, bs), bf16),
            pltpu.VMEM((2, 2, nb, LANES, bs), bf16),
            pltpu.VMEM((2, 2, quads + 1, nb * w, LANES), bf16),
            pltpu.VMEM((2, 4 * w, nb * bs), bf16),
            pltpu.VMEM((R, 2 * narrow, LANES), f32),
            pltpu.VMEM((R, packed, LANES), f32),
            pltpu.VMEM((R, n // 2, LANES), f32),
            pltpu.VMEM((2 * narrow, LANES), f32),
            pltpu.VMEM((packed, LANES), f32),
            pltpu.VMEM((n // 2, LANES), f32),
            pltpu.VMEM((3, R * w, LANES), f32),
            pltpu.VMEM((R * w, LANES), f32),
            pltpu.VMEM((2, 2, R * LANES, LANES), bf16),
            pltpu.VMEM((n, nb * bs), f32),
            pltpu.SemaphoreType.DMA((6,)),
            pltpu.SemaphoreType.DMA((2, nb)),
            pltpu.SemaphoreType.DMA((3, R)),
            pltpu.SemaphoreType.DMA((3, R)),
        ],
        compiler_params=pltpu.CompilerParams(
            collective_id=0, has_side_effects=True, vmem_limit_bytes=33554432
        ),
    )(*[pltpu.with_memory_space_constraint(a, pltpu.HBM) for a in (rhs, linv, flip(lleft), flip(lright), uinv, flip(uleft), flip(uright), ranks)])


def solution(mesh):
    blocks = P("rows", None, None)
    placed = (P("rhs", "rows"),) + (blocks,) * 6 + (P(None, "rows"),)
    return jax.shard_map(
        functools.partial(local, mesh.shape["rows"]),
        mesh=mesh,
        in_specs=placed,
        out_specs=(P("rhs", "rows"), P("rhs", "rows")),
        check_vma=False,
    )
```

```python
import functools

import jax
import jax.numpy as jnp
from jax import lax
from jax.experimental import pallas as pl
from jax.experimental.pallas import tpu as pltpu
from jax.sharding import PartitionSpec as P

MESH = pl.DeviceIdType.MESH
LANES = 128
f32, bf16 = jnp.float32, jnp.bfloat16


def split(x):
    hi = x.astype(bf16)
    return hi, (x - hi.astype(f32)).astype(bf16)


def dot(a, b):
    return jnp.dot(a, b, preferred_element_type=f32)


def dot_nt(a, b):
    return lax.dot_general(a, b, (((1,), (1,)), ((), ())), preferred_element_type=f32)


def dot_wide(a, b):
    r = dot(a, jnp.concatenate(split(b), axis=1))
    return r[:, :LANES] + r[:, LANES:]


def each(count, body):
    if count <= 8:
        for i in range(count):
            body(i)
    else:
        lax.fori_loop(0, count, lambda i, c: (body(i), c)[1], 0)


def rows_lanes(rows):
    return lax.broadcasted_iota(jnp.int32, (rows, LANES), 1)


def invert(qs, w):
    count = len(qs)
    lane = rows_lanes(w)
    row = lax.broadcasted_iota(jnp.int32, (w, LANES), 0)
    per = LANES // w
    tiles = count // per
    zero = jnp.zeros((w, LANES), f32)
    out = [[zero] * tiles for _ in range(count)]
    groups = []
    for b in range(count):
        home = jnp.where(lane == row + (b % per) * w, 1.0, 0.0)
        groups.append(([b], [qs[b]], -qs[b], {b // per: home}))
    while len(groups) > 1:
        merged = []
        last = len(groups) == 2
        for (ia, ra, da, ga), (ib, rb, db, gb) in zip(groups[::2], groups[1::2]):
            lhs = jnp.concatenate([*rb, db], axis=0).astype(bf16)[:, :w]
            tags = sorted(ga)
            rhs = jnp.concatenate([da] + [ga[t] for t in tags], axis=1).astype(bf16)
            res = dot(lhs, rhs)
            for i, b in enumerate(ib):
                for j, t in enumerate(tags):
                    part = res[w * i : w * (i + 1), LANES * (j + 1) : LANES * (j + 2)]
                    out[b][t] = out[b][t] - part
            if last:
                continue
            tail = w * len(ib)
            moved = [rb[i] + res[w * i : w * (i + 1), :LANES] for i in range(len(ib))]
            g = {t: ga[t] + res[tail:, LANES * (j + 1) : LANES * (j + 2)] for j, t in enumerate(tags)}
            for t in gb:
                g[t] = g[t] + gb[t] if t in g else gb[t]
            merged.append((ia + ib, ra + moved, da + db + res[tail:, :LANES], g))
        groups = merged
        if last:
            break
    return jnp.concatenate(
        [jnp.concatenate(parts, axis=1) for parts in out], axis=0
    ).astype(bf16)


def kernel(
    R, nb, bs, w, n,
    rhs_h, linv_h, llt_h, lrt_h, uinv_h, ult_h, urt_h, ranks_h,
    first, second,
    rhs, llt, lrt, ult, urt, ranks,
    inv, cm, wp, y, x1, x2, t1, t2, send0, send1, got0, got1, states,
    load_sem, block_sem, send_sem, recv_sem,
):
    me = lax.axis_index("rows")
    small = [
        pltpu.make_async_copy(src, dst, load_sem.at[i])
        for i, (src, dst) in enumerate(
            ((llt_h, llt), (lrt_h, lrt), (ranks_h, ranks), (rhs_h, rhs), (ult_h, ult), (urt_h, urt))
        )
    ]
    large = [
        [
            pltpu.make_async_copy(src.at[b], inv.at[f, b, 0:bs], block_sem.at[f, b])
            for b in (range(nb) if f == 0 else reversed(range(nb)))
        ]
        for f, src in ((0, linv_h), (1, uinv_h))
    ]
    for cp in small[:4] + large[0] + small[4:] + large[1]:
        cp.start()

    barrier = pltpu.get_barrier_semaphore()

    def greet(i):
        pl.semaphore_signal(
            barrier, inc=1, device_id={"rows": lax.rem(me + i + 1, R)}, device_id_type=MESH
        )

    each(R - 1, greet)

    lane = rows_lanes(w)
    row = lax.broadcasted_iota(jnp.int32, (w, LANES), 0)
    eye = jnp.where(lane == row, 1.0, 0.0)
    a_end, v_end = w, w + n
    zero = jnp.zeros((w, LANES), f32)

    def block(f, p):
        return p if f == 0 else nb - 1 - p

    def between(rows, lo, hi):
        l = rows_lanes(rows)
        return (l >= lo) & (l < hi)

    def part(x, p):
        return x[p * w : (p + 1) * w]

    lefts, rights = (llt, ult), (lrt, urt)

    def prepare(f):
        qs, us, pushed = [], [], {}
        wide_row = lax.broadcasted_iota(jnp.int32, (w, bs), 0)
        for p in range(nb):
            b = block(f, p)
            large[f][p].wait()
            base = inv[f, b, 0:bs]
            mt = jnp.where(wide_row < ranks[f, b], rights[f][b].astype(f32), 0.0).astype(bf16)
            if f == 0:
                z = dot_nt(base, jnp.concatenate([lefts[f][b], rhs[:, b * bs : (b + 1) * bs]], axis=0))
            else:
                z = dot_nt(base, lefts[f][b])
            z = jnp.concatenate([z, jnp.zeros((bs, LANES - z.shape[1]), f32)], axis=1)
            hi, lo = split(z)
            cm[f, b] = hi
            if f == 0:
                lo = jnp.where(rows_lanes(bs) < w, jnp.zeros_like(lo), lo)
                r = dot(mt, jnp.concatenate([hi, lo], axis=1))
                r = r[:, :LANES] + r[:, LANES:]
                pushed[b] = jnp.where(rows_lanes(bs) < w, 0.0, z)
            else:
                r = dot(mt, hi)
            qs.append(jnp.where(lane < w, r, 0.0))
            us.append(jnp.where(lane < w, -r, r))
            hi, lo = split(dot(mt, base))
            inv[f, b, bs : bs + w] = hi
            inv[f, b, bs + w : bs + 2 * w] = lo
        return qs, us, pushed

    def advance(f, us):
        u = jnp.concatenate(us, axis=0)
        return u + dot(wp[f], u.astype(bf16))

    def total(x, count):
        s = part(x, 0)
        for p in range(1, count):
            s = s + part(x, p)
        return s

    def coupled(f, b, s):
        return dot_wide(cm[f, b][:, :w], s)

    def push(f, src):
        us, pushed = [], {}
        for p in range(nb):
            b = block(f, p)
            r = dot_wide(inv[f, b], src[b])
            pushed[b] = r[:bs]
            us.append(r[bs : bs + w] + r[bs + w :])
        return advance(f, us), pushed

    def solve(f, wv, pushed, dst, plus=None):
        s = None
        for p in range(nb):
            b = block(f, p)
            out = pushed[b]
            if s is not None:
                out = out - coupled(f, b, s)
            if plus is not None:
                out = out + plus(b)
            dst[b] = out
            s = part(wv, p) if s is None else s + part(wv, p)

    for cp in small[:4]:
        cp.wait()
    qs, us, pushed = prepare(0)
    wp[0] = invert(qs, w)
    w_a = advance(0, us)
    end_a = total(w_a, nb)
    s = eye
    for p in range(nb):
        y[p] = pushed[p] - coupled(0, p, s)
        s = s + part(w_a, p)

    for cp in small[4:]:
        cp.wait()
    qs, us, _ = prepare(1)
    wp[1] = invert(qs, w)
    w_u = advance(1, us)
    end_u = jnp.where(lane < w, total(w_u, nb), 0.0)
    s = eye
    for p in range(nb):
        b = block(1, p)
        x1[b] = -coupled(1, b, pltpu.roll(s, v_end, 1))
        s = s + jnp.where(lane < w, part(w_u, p), 0.0)

    w_b, pushed = push(1, y)
    end_b = total(w_b, nb)
    tile0 = (
        jnp.where(lane < v_end, end_a, 0.0)
        + pltpu.roll(end_u, v_end, 1)
        + pltpu.roll(jnp.where(lane < v_end, end_b, 0.0), v_end + w, 1)
    )
    send0[...] = tile0.astype(bf16)

    def copy(k, src, dst, i):
        peer = lax.rem(me + i + 1, R)
        return pltpu.make_async_remote_copy(
            src_ref=src, dst_ref=dst.at[me], send_sem=send_sem.at[k, i],
            recv_sem=recv_sem.at[k, me], device_id={"rows": peer}, device_id_type=MESH,
        )

    def arrive(k, src, dst, i):
        peer = lax.rem(me + i + 1, R)
        pltpu.make_async_remote_copy(
            src_ref=src, dst_ref=dst.at[peer], send_sem=send_sem.at[k, i],
            recv_sem=recv_sem.at[k, peer], device_id={"rows": peer}, device_id_type=MESH,
        ).wait_recv()

    pl.semaphore_wait(barrier, R - 1)
    each(R - 1, lambda i: copy(0, send0, got0, i).start())
    got0[me] = send0[...]

    solve(1, w_b, pushed, x1, plus=lambda b: x1[b])
    w_c, pushed = push(0, x1)
    send1[:w] = total(w_c, nb).astype(bf16)
    solve(0, w_c, pushed, y)
    w_d, pushed = push(1, y)
    send1[w:] = total(w_d, nb).astype(bf16)
    each(R - 1, lambda i: copy(1, send1, got1, i).start())
    got1[me] = send1[...]

    solve(1, w_d, pushed, x2)

    def flip(src, dst):
        for b in range(nb):
            hi, lo = split(src[b].T)
            dst[b, :LANES] = hi
            dst[b, LANES:] = lo

    flip(x1, t1)
    flip(x2, t2)

    spot = jnp.where((lane == row + w) & (row < n), 1.0, 0.0)[:n]
    gap_n = jnp.zeros((n, LANES), f32)

    def stack(a, v, u, b, t):
        parts = [zero if a is None else a, gap_n if v is None else v, zero if u is None else u]
        parts += [zero if b is None else b, gap_n if t is None else t]
        return jnp.concatenate(parts, axis=0)

    def times(tile, x):
        hi, lo = split(x)
        return dot(tile, hi) + dot(tile, lo)

    each(R - 1, lambda i: arrive(0, send0, got0, i))
    if R <= 8:
        def sweep(wv, order):
            s, out = zero, [None] * R
            for i, d in enumerate(order):
                out[d] = s
                s = s + part(wv, i)
            return out

        up, down = list(range(R)), list(range(R - 1, -1, -1))
        tiles = [got0[d] for d in range(R)]
        wide = [t.astype(f32) for t in tiles]
        inner = lane < w
        fwd = invert([jnp.where(inner, -wide[d], 0.0) for d in up], w)
        bwd = invert(
            [jnp.where(inner, -pltpu.roll(wide[d], LANES - v_end, 1), 0.0) for d in down], w
        )

        def carry(m, inverse, order):
            u = jnp.concatenate([m[d] for d in order], axis=0)
            return sweep(u + dot(inverse, u.astype(bf16)), order)

        mid = between(w, w, v_end)
        s1 = carry([jnp.where(mid, wide[d], 0.0) for d in up], fwd, up)
        m2 = [dot(tiles[d], stack(None, None, None, s1[d], spot).astype(bf16)) for d in up]
        s2 = carry(m2, bwd, down)
        for d in up:
            states[0, d * w : (d + 1) * w] = s1[d]
            states[1, d * w : (d + 1) * w] = s2[d]
        each(R - 1, lambda i: arrive(1, send1, got1, i))
        m34 = [dot(got1[d], stack(s1[d], spot, s2[d], None, None).astype(bf16)) for d in up]
        s3 = carry([m34[d][:w] for d in up], fwd, up)
        m4 = [
            m34[d][w:] + dot(tiles[d], stack(None, None, None, s3[d], None).astype(bf16))
            for d in up
        ]
        s4 = carry(m4, bwd, down)
        for d in up:
            states[2, d * w : (d + 1) * w] = s3[d]
            states[3, d * w : (d + 1) * w] = s4[d]
    else:
        each(R - 1, lambda i: arrive(1, send1, got1, i))

        def at(d):
            return pl.ds(pl.multiple_of(d * w, w), w)

        def walk(k, step, back):
            def body(i, s):
                d = R - 1 - i if back else i
                states[k, at(d)] = s
                return s + step(d, s)

            lax.fori_loop(0, R, body, zero)

        def joint(d):
            return stack(states[0, at(d)], spot, states[1, at(d)], None, None)

        walk(0, lambda d, s: times(got0[d], stack(s, spot, None, None, None)), False)
        walk(1, lambda d, s: times(got0[d], stack(None, None, s, states[0, at(d)], spot)), True)
        walk(
            2,
            lambda d, s: times(got1[d, :w], joint(d))
            + times(got0[d], stack(s, None, None, None, None)),
            False,
        )
        walk(
            3,
            lambda d, s: times(got1[d, w:], joint(d))
            + times(got0[d], stack(None, None, s, states[2, at(d)], None)),
            True,
        )

    mine = pl.ds(pl.multiple_of(me * w, w), w)
    own = [states[k, mine] for k in range(4)]

    def weights(x):
        hi, lo = split(x.T[w:v_end])
        both = jnp.concatenate([hi, lo], axis=0)
        return jnp.concatenate([both, both], axis=1)

    one = weights(stack(own[0], spot, own[1], None, None))
    two = weights(stack(own[2], None, own[3], None, None))
    lhs = jnp.concatenate([one, two], axis=0)
    for b in range(nb):
        r = dot(lhs, t1[b])
        q = dot(one, t2[b])
        first[:, b * bs : (b + 1) * bs] = r[:n] + r[n : 2 * n]
        second[:, b * bs : (b + 1) * bs] = r[2 * n : 3 * n] + r[3 * n :] + q[:n] + q[n:]

    each(R - 1, lambda i: copy(0, send0, got0, i).wait_send())
    each(R - 1, lambda i: copy(1, send1, got1, i).wait_send())


def local(R, rhs, linv, lleft, lright, uinv, uleft, uright, ranks):
    nb, bs, w = lleft.shape
    n = rhs.shape[0]
    flip = lambda a: jnp.swapaxes(a, 1, 2)
    vmem = pl.BlockSpec(memory_space=pltpu.VMEM)
    hbm = pl.BlockSpec(memory_space=pltpu.HBM)
    out = jax.ShapeDtypeStruct(rhs.shape, f32)
    slim = pltpu.VMEM((nb, w, bs), bf16)
    tall = pltpu.VMEM((nb, bs, LANES), f32)
    args = (rhs, linv, flip(lleft), flip(lright), uinv, flip(uleft), flip(uright), ranks)
    return pl.pallas_call(
        functools.partial(kernel, R, nb, bs, w, n),
        out_shape=(out, out),
        in_specs=[hbm] * 8,
        out_specs=(vmem, vmem),
        scratch_shapes=[
            pltpu.VMEM(rhs.shape, bf16),
            slim, slim, slim, slim,
            pltpu.SMEM(ranks.shape, jnp.int32),
            pltpu.VMEM((2, nb, bs + 2 * w, bs), bf16),
            pltpu.VMEM((2, nb, bs, LANES), bf16),
            pltpu.VMEM((2, nb * w, nb * w), bf16),
            tall, tall, tall,
            pltpu.VMEM((nb, 2 * LANES, bs), bf16),
            pltpu.VMEM((nb, 2 * LANES, bs), bf16),
            pltpu.VMEM((w, LANES), bf16),
            pltpu.VMEM((2 * w, LANES), bf16),
            pltpu.VMEM((R, w, LANES), bf16),
            pltpu.VMEM((R, 2 * w, LANES), bf16),
            pltpu.VMEM((4, R * w, LANES), f32),
            pltpu.SemaphoreType.DMA((6,)),
            pltpu.SemaphoreType.DMA((2, nb)),
            pltpu.SemaphoreType.DMA((2, R)),
            pltpu.SemaphoreType.DMA((2, R)),
        ],
        compiler_params=pltpu.CompilerParams(
            collective_id=0, has_side_effects=True, vmem_limit_bytes=33554432
        ),
    )(*[pltpu.with_memory_space_constraint(a, pltpu.HBM) for a in args])


def solution(mesh):
    blocks = P("rows", None, None)
    placed = (P("rhs", "rows"),) + (blocks,) * 6 + (P(None, "rows"),)
    return jax.shard_map(
        functools.partial(local, mesh.shape["rows"]),
        mesh=mesh,
        in_specs=placed,
        out_specs=(P("rhs", "rows"), P("rhs", "rows")),
        check_vma=False,
    )
```

```python
import functools

import jax
import jax.numpy as jnp
from jax import lax
from jax.experimental import pallas as pl
from jax.experimental.pallas import tpu as pltpu
from jax.sharding import PartitionSpec as P

MESH = pl.DeviceIdType.MESH
LANES = 128
f32, bf16 = jnp.float32, jnp.bfloat16


def split(x):
    hi = x.astype(bf16)
    return hi, (x - hi.astype(f32)).astype(bf16)


def dot(a, b):
    return jnp.dot(a, b, preferred_element_type=f32)


def dot_nt(a, b):
    return lax.dot_general(a, b, (((1,), (1,)), ((), ())), preferred_element_type=f32)


def each(count, body):
    if count <= 8:
        for i in range(count):
            body(i)
    else:
        lax.fori_loop(0, count, lambda i, c: (body(i), c)[1], 0)


def rows_lanes(rows):
    return lax.broadcasted_iota(jnp.int32, (rows, LANES), 1)


def invert_steps(qs, w, out):
    count = len(qs)
    lane = rows_lanes(w)
    row = lax.broadcasted_iota(jnp.int32, (w, LANES), 0)
    per = LANES // w
    tiles = count // per
    zero = jnp.zeros((w, LANES), f32)
    out.extend([zero] * tiles for _ in range(count))
    groups = []
    for b in range(count):
        home = jnp.where(lane == row + (b % per) * w, 1.0, 0.0)
        groups.append(([b], [qs[b]], -qs[b], {b // per: home}))
    while len(groups) > 1:
        merged = []
        last = len(groups) == 2
        for (ia, ra, da, ga), (ib, rb, db, gb) in zip(groups[::2], groups[1::2]):
            lhs = jnp.concatenate(rb if last else [*rb, db], axis=0).astype(bf16)[:, :w]
            tags = sorted(ga)
            rhs = jnp.concatenate([ga[t] for t in tags] + ([] if last else [da]), axis=1).astype(bf16)
            res = dot(lhs, rhs)
            at = len(tags) * LANES
            for i, b in enumerate(ib):
                for j, t in enumerate(tags):
                    out[b][t] = out[b][t] - res[w * i : w * (i + 1), LANES * j : LANES * (j + 1)]
            if last:
                continue
            tail = w * len(ib)
            moved = [rb[i] + res[w * i : w * (i + 1), at:] for i in range(len(ib))]
            g = {t: ga[t] + res[tail:, LANES * j : LANES * (j + 1)] for j, t in enumerate(tags)}
            for t in gb:
                g[t] = g[t] + gb[t] if t in g else gb[t]
            merged.append((ia + ib, ra + moved, da + db + res[tail:, at:], g))
        groups = merged
        yield
        if last:
            break


def together(*steps):
    live = list(steps)
    while live:
        live = [s for s in live if next(s, s) is not s]


def joined(out):
    return jnp.concatenate([jnp.concatenate(parts, axis=1) for parts in out], axis=0)


def kernel(
    R, nb, bs, w, n,
    rhs_h, linv_h, llt_h, lrt_h, uinv_h, ult_h, urt_h, ranks_h,
    first, second,
    rhs, llt, lrt, ult, urt, ranks,
    inv, cm, wp, y, x1, x2, t1, t2, send0, send1, got0, got1, states,
    load_sem, block_sem, send_sem, recv_sem,
):
    me = lax.axis_index("rows")
    small = [
        pltpu.make_async_copy(src, dst, load_sem.at[i])
        for i, (src, dst) in enumerate(
            ((lrt_h, lrt), (ranks_h, ranks), (llt_h, llt), (rhs_h, rhs), (urt_h, urt), (ult_h, ult))
        )
    ]
    large = [
        [
            pltpu.make_async_copy(src.at[b], inv.at[f, b, 0:bs], block_sem.at[f, b])
            for b in range(nb)
        ]
        for f, src in ((0, linv_h), (1, uinv_h))
    ]
    for cp in small[:4] + large[0] + small[4:] + large[1]:
        cp.start()

    barrier = pltpu.get_barrier_semaphore()

    def greet(i):
        pl.semaphore_signal(
            barrier, inc=1, device_id={"rows": lax.rem(me + i + 1, R)}, device_id_type=MESH
        )

    each(R - 1, greet)

    lane = rows_lanes(w)
    row = lax.broadcasted_iota(jnp.int32, (w, LANES), 0)
    v_at, lo_at, v_end = 2 * w, 2 * w + n, 2 * w + 2 * n
    zero = jnp.zeros((w, LANES), f32)
    gap = jnp.zeros((n, LANES), f32)
    eye_l = jnp.where(lane == row, 1.0, 0.0)
    eye_u = jnp.where(lane == row + w, 1.0, 0.0)
    n_hi, n_lo, adj = bs, bs + w, bs + 2 * w

    def block(f, p):
        return p if f == 0 else nb - 1 - p

    def between(rows, lo, hi):
        l = rows_lanes(rows)
        return (l >= lo) & (l < hi)

    def part(x, p):
        return x[p * w : (p + 1) * w]

    lefts, rights = (llt, ult), (lrt, urt)

    def reduce_left(f):
        wide_row = lax.broadcasted_iota(jnp.int32, (w, bs), 0)
        tall = []
        for p in range(nb):
            b = block(f, p)
            mt = jnp.where(wide_row < ranks[f, b], rights[f][b].astype(f32), 0.0).astype(bf16)
            t = dot(mt, inv[f, b, 0:bs])
            hi, lo = split(t)
            inv[f, b, n_hi:n_lo] = hi
            inv[f, b, n_lo:adj] = lo
            tall.append(t)
        return tall

    def prepare(f):
        qs, us, pushed = [], [], {}
        for p in range(nb):
            b = block(f, p)
            left = lefts[f][b]
            if f == 0:
                v = rhs[:, b * bs : (b + 1) * bs]
                cols = jnp.concatenate([left, left, v, v], axis=0)
            else:
                cols = jnp.concatenate([left, left], axis=0)
            z = dot_nt(inv[f, b, 0:adj], cols)
            z = jnp.concatenate([z, jnp.zeros((adj, LANES - z.shape[1]), f32)], axis=1)
            cm[f, b] = z[:bs].astype(bf16)
            pushed[b] = z[:bs]
            r = z[n_hi:n_lo] + z[n_lo:]
            qs.append(jnp.where(lane < w, r, 0.0))
            if f == 0:
                us.append(jnp.where(lane < w, -r, jnp.where(lane < v_at, 0.0, r)))
            else:
                us.append(jnp.where((lane >= w) & (lane < v_at), -r, 0.0))
        return qs, us, pushed

    def advance(f, us):
        u = jnp.concatenate(us, axis=0)
        return u + dot(wp[f], u.astype(bf16))

    def total(x, count):
        s = part(x, 0)
        for p in range(1, count):
            s = s + part(x, p)
        return s

    def coupled(f, b, s):
        return dot(cm[f, b][:, : 2 * w], jnp.concatenate(split(s), axis=0))

    def push(f, src, count):
        us, pushed = [], {}
        for p in range(nb):
            b = block(f, p)
            r = dot(inv[f, b, 0:adj], src(b))
            pushed[b] = r[:bs]
            us.append(r[n_hi:n_lo] + r[n_lo:])
        return us, pushed

    def solve(f, wv, pushed, dst, s=None):
        for p in range(nb):
            b = block(f, p)
            dst[b] = pushed[b] if s is None else pushed[b] - coupled(f, b, s)
            s = part(wv, p) if s is None else s + part(wv, p)

    def columns(x):
        hi = x.astype(bf16)
        l = rows_lanes(bs)
        rest = x - hi.astype(f32)
        low = jnp.where(between(bs, lo_at, v_end), x + pltpu.roll(rest, n, 1), x)
        return low.astype(bf16)

    for cp in small[:2]:
        cp.wait()
    for cp in small[2:4]:
        cp.wait()
    for cp in large[0]:
        cp.wait()
    reduce_left(0)
    for cp in small[4:]:
        cp.wait()
    for cp in large[1]:
        cp.wait()
    tall_u = reduce_left(1)
    qs_l, us_l, z_l = prepare(0)
    qs_u, us_u, _ = prepare(1)
    out_l, out_u = [], []
    together(invert_steps(qs_l, w, out_l), invert_steps(qs_u, w, out_u))
    wp[0] = joined(out_l).astype(bf16)
    dev_u = joined(out_u)
    wp[1] = dev_u.astype(bf16)
    w_a = advance(0, us_l)
    w_u = advance(1, us_u)

    top = total(dev_u, nb)
    spread = jnp.concatenate([top] * nb, axis=0)
    r_id = lax.broadcasted_iota(jnp.int32, spread.shape, 0) // w
    c_id = lax.broadcasted_iota(jnp.int32, spread.shape, 1) // w
    stacked = jnp.concatenate(tall_u, axis=0)
    adjoint = stacked + dot(
        jnp.where(r_id == c_id, spread, 0.0).astype(bf16), stacked.astype(bf16)
    )
    turn = {}

    s = eye_l
    for p in range(nb):
        y[p] = jnp.where(between(bs, v_at, v_end), z_l[p], 0.0) - coupled(0, p, s)
        s = s + part(w_a, p)
        b = p
        a = part(adjoint, block(1, b)).astype(bf16)
        inv[0, b, adj:] = dot(a, inv[0, b, 0:bs]).astype(bf16)
        turn[b] = dot(a, cm[0, b]).astype(bf16)[:, :w]

    def twin(b):
        x = y[b]
        hi = x.astype(bf16)
        return jnp.where(between(bs, lo_at, v_end), x - hi.astype(f32), x).astype(bf16)

    us, pushed = push(1, twin, nb)
    w_b = advance(1, us)
    end_a, end_u, end_b = total(w_a, nb), total(w_u, nb), total(w_b, nb)
    shift = pltpu.roll(end_b, n, 1)
    tile0 = jnp.where(lane < w, end_a, end_u)
    tile0 = jnp.where(between(w, v_at, lo_at), end_a, tile0)
    tile0 = jnp.where(between(w, lo_at, v_end), end_b + shift, tile0)
    tile0 = jnp.where(lane >= v_end, pltpu.roll(end_b, v_end, 1), tile0)
    send0[...] = tile0.astype(bf16)

    def copy(k, src, dst, i):
        peer = lax.rem(me + i + 1, R)
        return pltpu.make_async_remote_copy(
            src_ref=src, dst_ref=dst.at[me], send_sem=send_sem.at[k, i],
            recv_sem=recv_sem.at[k, me], device_id={"rows": peer}, device_id_type=MESH,
        )

    def arrive(k, src, dst, i):
        peer = lax.rem(me + i + 1, R)
        pltpu.make_async_remote_copy(
            src_ref=src, dst_ref=dst.at[peer], send_sem=send_sem.at[k, i],
            recv_sem=recv_sem.at[k, peer], device_id={"rows": peer}, device_id_type=MESH,
        ).wait_recv()

    pl.semaphore_wait(barrier, R - 1)
    each(R - 1, lambda i: copy(0, send0, got0, i).start())
    got0[me] = send0[...]

    solve(1, w_b + w_u, pushed, x1, eye_u)
    us, direct = [], None
    for b in range(nb):
        r = dot(inv[0, b, n_hi:], x1[b].astype(bf16))
        us.append(r[:w] + r[w : 2 * w])
        direct = r[2 * w :] if direct is None else direct + r[2 * w :]
    w_c = advance(0, us)
    send1[:w] = total(w_c, nb).astype(bf16)
    s = part(w_c, 0)
    crossed = None
    for b in range(1, nb):
        t = dot(turn[b], s.astype(bf16))
        crossed = t if crossed is None else crossed + t
        s = s + part(w_c, b)
    send1[w:] = (direct - crossed).astype(bf16)
    each(R - 1, lambda i: copy(1, send1, got1, i).start())
    got1[me] = send1[...]

    us, pushed = push(0, lambda b: columns(x1[b]), nb)
    solve(0, advance(0, us), pushed, y)
    us, pushed = push(1, lambda b: columns(y[b]), nb)
    solve(1, advance(1, us), pushed, x2)

    def flip(src, dst):
        for b in range(nb):
            hi, lo = split(src[b].T)
            dst[b, :LANES] = hi
            dst[b, LANES:] = lo

    flip(x1, t1)
    flip(x2, t2)

    spot = jnp.where((lane == row + v_at) & (row < n), 1.0, 0.0)[:n]

    def near(a, b, own):
        a, b = (zero if a is None else a), (zero if b is None else b)
        v = spot if own else gap
        return jnp.concatenate([a, b, v, v, zero], axis=0)

    def late(b, own, a=None):
        return jnp.concatenate(
            [zero, zero if a is None else a, gap, spot if own else gap, b], axis=0
        )

    def times(tile, x):
        hi, lo = split(x)
        return dot(tile, hi) + dot(tile, lo)

    def weights(x):
        hi, lo = split(x.T[v_at:lo_at])
        both = jnp.concatenate([hi, lo], axis=0)
        return jnp.concatenate([both, both], axis=1)

    def halves(r):
        return r[:n] + r[n:]

    mine = pl.ds(pl.multiple_of(me * w, w), w)

    def opening():
        one = weights(near(states[0, mine], states[1, mine], True))
        for b in range(nb):
            at = slice(b * bs, (b + 1) * bs)
            first[:, at] = halves(dot(one, t1[b]))
            second[:, at] = halves(dot(one, t2[b]))

    each(R - 1, lambda i: arrive(0, send0, got0, i))
    if R <= 8:
        def sweep(wv, order):
            s, out = zero, [None] * R
            for i, d in enumerate(order):
                out[d] = s
                s = s + part(wv, i)
            return out

        up, down = list(range(R)), list(range(R - 1, -1, -1))
        tiles = [got0[d] for d in range(R)]
        wide = [t.astype(f32) for t in tiles]
        inner = lane < w
        out_f, out_b = [], []
        together(
            invert_steps([jnp.where(inner, -wide[d], 0.0) for d in up], w, out_f),
            invert_steps(
                [jnp.where(inner, -pltpu.roll(wide[d], LANES - w, 1), 0.0) for d in down], w, out_b
            ),
        )
        fwd, bwd = joined(out_f).astype(bf16), joined(out_b).astype(bf16)

        def carry(m, inverse, order):
            u = jnp.concatenate([m[d] for d in order], axis=0)
            return sweep(u + dot(inverse, u.astype(bf16)), order)

        mid = between(w, v_at, lo_at)
        s1 = carry([jnp.where(mid, wide[d], 0.0) for d in up], fwd, up)
        m2 = [dot(tiles[d], late(s1[d], True).astype(bf16)) for d in up]
        s2 = carry(m2, bwd, down)
        for d in up:
            states[0, d * w : (d + 1) * w] = s1[d]
            states[1, d * w : (d + 1) * w] = s2[d]
        opening()
        each(R - 1, lambda i: arrive(1, send1, got1, i))
        m34 = [dot(got1[d], near(s1[d], s2[d], True).astype(bf16)) for d in up]
        s3 = carry([m34[d][:w] for d in up], fwd, up)
        m4 = [m34[d][w:] + dot(tiles[d], late(s3[d], False).astype(bf16)) for d in up]
        s4 = carry(m4, bwd, down)
        for d in up:
            states[2, d * w : (d + 1) * w] = s3[d]
            states[3, d * w : (d + 1) * w] = s4[d]
    else:
        def at(d):
            return pl.ds(pl.multiple_of(d * w, w), w)

        def walk(k, step, back):
            def body(i, s):
                d = R - 1 - i if back else i
                states[k, at(d)] = s
                return s + step(d, s)

            lax.fori_loop(0, R, body, zero)

        def joint(d):
            return near(states[0, at(d)], states[1, at(d)], True)

        def ahead(s, own):
            v = spot if own else gap
            return jnp.concatenate([s, zero, v, gap, zero], axis=0)

        walk(0, lambda d, s: times(got0[d], ahead(s, True)), False)
        walk(1, lambda d, s: times(got0[d], late(states[0, at(d)], True, s)), True)
        opening()
        each(R - 1, lambda i: arrive(1, send1, got1, i))
        walk(
            2,
            lambda d, s: times(got1[d, :w], joint(d)) + times(got0[d], ahead(s, False)),
            False,
        )
        walk(
            3,
            lambda d, s: times(got1[d, w:], joint(d))
            + times(got0[d], late(states[2, at(d)], False, s)),
            True,
        )

    two = weights(near(states[2, mine], states[3, mine], False))
    for b in range(nb):
        at = slice(b * bs, (b + 1) * bs)
        second[:, at] = second[:, at] + halves(dot(two, t1[b]))

    each(R - 1, lambda i: copy(0, send0, got0, i).wait_send())
    each(R - 1, lambda i: copy(1, send1, got1, i).wait_send())


def local(R, rhs, linv, lleft, lright, uinv, uleft, uright, ranks):
    nb, bs, w = lleft.shape
    n = rhs.shape[0]
    flip = lambda a: jnp.swapaxes(a, 1, 2)
    vmem = pl.BlockSpec(memory_space=pltpu.VMEM)
    hbm = pl.BlockSpec(memory_space=pltpu.HBM)
    out = jax.ShapeDtypeStruct(rhs.shape, f32)
    slim = pltpu.VMEM((nb, w, bs), bf16)
    tall = pltpu.VMEM((nb, bs, LANES), f32)
    args = (rhs, linv, flip(lleft), flip(lright), uinv, flip(uleft), flip(uright), ranks)
    return pl.pallas_call(
        functools.partial(kernel, R, nb, bs, w, n),
        out_shape=(out, out),
        in_specs=[hbm] * 8,
        out_specs=(vmem, vmem),
        scratch_shapes=[
            pltpu.VMEM(rhs.shape, bf16),
            slim, slim, slim, slim,
            pltpu.SMEM(ranks.shape, jnp.int32),
            pltpu.VMEM((2, nb, bs + 3 * w, bs), bf16),
            pltpu.VMEM((2, nb, bs, LANES), bf16),
            pltpu.VMEM((2, nb * w, nb * w), bf16),
            tall, tall, tall,
            pltpu.VMEM((nb, 2 * LANES, bs), bf16),
            pltpu.VMEM((nb, 2 * LANES, bs), bf16),
            pltpu.VMEM((w, LANES), bf16),
            pltpu.VMEM((2 * w, LANES), bf16),
            pltpu.VMEM((R, w, LANES), bf16),
            pltpu.VMEM((R, 2 * w, LANES), bf16),
            pltpu.VMEM((4, R * w, LANES), f32),
            pltpu.SemaphoreType.DMA((6,)),
            pltpu.SemaphoreType.DMA((2, nb)),
            pltpu.SemaphoreType.DMA((2, R)),
            pltpu.SemaphoreType.DMA((2, R)),
        ],
        compiler_params=pltpu.CompilerParams(
            collective_id=0, has_side_effects=True, vmem_limit_bytes=33554432
        ),
    )(*[pltpu.with_memory_space_constraint(a, pltpu.HBM) for a in args])


def solution(mesh):
    blocks = P("rows", None, None)
    placed = (P("rhs", "rows"),) + (blocks,) * 6 + (P(None, "rows"),)
    return jax.shard_map(
        functools.partial(local, mesh.shape["rows"]),
        mesh=mesh,
        in_specs=placed,
        out_specs=(P("rhs", "rows"), P("rhs", "rows")),
        check_vma=False,
    )
```

```python
import functools

import jax
import jax.numpy as jnp
from jax import lax
from jax.experimental import pallas as pl
from jax.experimental.pallas import tpu as pltpu
from jax.sharding import PartitionSpec as P

MESH = pl.DeviceIdType.MESH
LANES = 128
f32, bf16 = jnp.float32, jnp.bfloat16


def split(x):
    hi = x.astype(bf16)
    return hi, (x - hi.astype(f32)).astype(bf16)


def dot(a, b):
    return jnp.dot(a, b, preferred_element_type=f32)


def dot_nt(a, b):
    return lax.dot_general(a, b, (((1,), (1,)), ((), ())), preferred_element_type=f32)


def each(count, body):
    if count <= 8:
        for i in range(count):
            body(i)
    else:
        lax.fori_loop(0, count, lambda i, c: (body(i), c)[1], 0)


def rows_lanes(rows):
    return lax.broadcasted_iota(jnp.int32, (rows, LANES), 1)


def invert_steps(qs, w, out):
    count = len(qs)
    lane = rows_lanes(w)
    row = lax.broadcasted_iota(jnp.int32, (w, LANES), 0)
    per = LANES // w
    tiles = count // per
    zero = jnp.zeros((w, LANES), f32)
    out.extend([zero] * tiles for _ in range(count))
    groups = []
    for b in range(count):
        home = jnp.where(lane == row + (b % per) * w, 1.0, 0.0)
        groups.append(([b], [qs[b]], -qs[b], {b // per: home}))
    while len(groups) > 1:
        merged = []
        last = len(groups) == 2
        for (ia, ra, da, ga), (ib, rb, db, gb) in zip(groups[::2], groups[1::2]):
            lhs = jnp.concatenate(rb if last else [*rb, db], axis=0).astype(bf16)[:, :w]
            tags = sorted(ga)
            rhs = jnp.concatenate([ga[t] for t in tags] + ([] if last else [da]), axis=1).astype(bf16)
            res = dot(lhs, rhs)
            at = len(tags) * LANES
            for i, b in enumerate(ib):
                for j, t in enumerate(tags):
                    out[b][t] = out[b][t] - res[w * i : w * (i + 1), LANES * j : LANES * (j + 1)]
            if last:
                continue
            tail = w * len(ib)
            moved = [rb[i] + res[w * i : w * (i + 1), at:] for i in range(len(ib))]
            g = {t: ga[t] + res[tail:, LANES * j : LANES * (j + 1)] for j, t in enumerate(tags)}
            for t in gb:
                g[t] = g[t] + gb[t] if t in g else gb[t]
            merged.append((ia + ib, ra + moved, da + db + res[tail:, at:], g))
        groups = merged
        yield
        if last:
            break


def together(*steps):
    live = list(steps)
    while live:
        live = [s for s in live if next(s, s) is not s]


def joined(out):
    return jnp.concatenate([jnp.concatenate(parts, axis=1) for parts in out], axis=0)


def kernel(
    R, nb, bs, w, n,
    rhs_h, linv_h, llt_h, lrt_h, uinv_h, ult_h, urt_h, ranks_h,
    first, second,
    rhs, llt, lrt, ult, urt, ranks,
    inv, adj, cm, wp, y, x1, x2, t1, t2, send0, send1, got0, got1, states, maps,
    load_sem, block_sem, send_sem, recv_sem,
):
    me = lax.axis_index("rows")
    small = [
        pltpu.make_async_copy(src, dst, load_sem.at[i])
        for i, (src, dst) in enumerate(
            ((lrt_h, lrt), (ranks_h, ranks), (llt_h, llt), (rhs_h, rhs), (urt_h, urt), (ult_h, ult))
        )
    ]
    large = [
        [
            pltpu.make_async_copy(src.at[b], inv.at[f, b, 0:bs], block_sem.at[f, b])
            for b in range(nb)
        ]
        for f, src in ((0, linv_h), (1, uinv_h))
    ]
    for cp in small[:4] + large[0] + small[4:] + large[1]:
        cp.start()

    barrier = pltpu.get_barrier_semaphore()

    def greet(i):
        pl.semaphore_signal(
            barrier, inc=1, device_id={"rows": lax.rem(me + i + 1, R)}, device_id_type=MESH
        )

    each(R - 1, greet)

    lane = rows_lanes(w)
    row = lax.broadcasted_iota(jnp.int32, (w, LANES), 0)
    v_at, lo_at, v_end = 2 * w, 2 * w + n, 2 * w + 2 * n
    zero = jnp.zeros((w, LANES), f32)
    gap = jnp.zeros((n, LANES), f32)
    eye_l = jnp.where(lane == row, 1.0, 0.0)
    eye_u = jnp.where(lane == row + w, 1.0, 0.0)
    low, full_rows = bs, bs + w

    def block(f, p):
        return p if f == 0 else nb - 1 - p

    def between(rows, lo, hi):
        l = rows_lanes(rows)
        return (l >= lo) & (l < hi)

    def part(x, p):
        return x[p * w : (p + 1) * w]

    lefts, rights = (llt, ult), (lrt, urt)

    def reduce_left(f):
        wide_row = lax.broadcasted_iota(jnp.int32, (w, bs), 0)
        tall = []
        for p in range(nb):
            b = block(f, p)
            mt = jnp.where(wide_row < ranks[f, b], rights[f][b].astype(f32), 0.0).astype(bf16)
            t = dot(mt, inv[f, b, 0:bs])
            inv[f, b, low:full_rows] = t.astype(bf16)
            tall.append(t)
        return tall

    def lead(f):
        qs, us = [], []
        for p in range(nb):
            b = block(f, p)
            cols = lefts[f][b]
            if f == 0:
                cols = jnp.concatenate([cols, rhs[:, b * bs : (b + 1) * bs]], axis=0)
            r = dot_nt(inv[f, b, low:full_rows], cols)
            r = jnp.concatenate([r, jnp.zeros((w, LANES - r.shape[1]), f32)], axis=1)
            qs.append(jnp.where(lane < w, r, 0.0))
            if f == 0:
                u = jnp.where(lane < w, -r, 0.0)
                u = jnp.where(between(w, v_at, lo_at), pltpu.roll(r, v_at - w, 1), u)
                us.append(jnp.where(between(w, lo_at, v_end), pltpu.roll(r, lo_at - w, 1), u))
            else:
                us.append(jnp.where(between(w, w, v_at), pltpu.roll(-r, w, 1), 0.0))
        return qs, us

    def couple(f, pushed, chunk):
        for p in range(nb):
            b = block(f, p)
            left = lefts[f][b]
            cols = [left, left]
            if f == 0:
                v = rhs[:, b * bs : (b + 1) * bs]
                cols += [v, v]
            z = dot_nt(inv[f, b, 0:bs], jnp.concatenate(cols, axis=0))
            z = jnp.concatenate([z, jnp.zeros((bs, LANES - z.shape[1]), f32)], axis=1)
            cm[f, b] = z.astype(bf16)
            pushed[b] = z
            if p % chunk == chunk - 1:
                yield

    per = LANES // w

    def diagonal(tiles):
        return jnp.concatenate(
            [
                jnp.concatenate(
                    [
                        jnp.where(lane // w == p % per, tiles[t], 0.0) if t == p // per else zero
                        for t in range(len(tiles))
                    ],
                    axis=1,
                )
                for p in range(len(tiles) * per)
            ],
            axis=0,
        ).astype(bf16)

    def tops(out):
        return [sum(out[p][t] for p in range(1, len(out))) for t in range(len(out[0]))]

    def home(p, t):
        return jnp.where(lane == row + p % per * w, 1.0, 0.0) if t == p // per else zero

    def advance(f, us):
        u = jnp.concatenate(us, axis=0)
        return u + dot(wp[f], u.astype(bf16))

    def total(x, count):
        s = part(x, 0)
        for p in range(1, count):
            s = s + part(x, p)
        return s

    def coupled(f, b, s):
        return dot(cm[f, b][:, : 2 * w], jnp.concatenate(split(s), axis=0))

    def push(f, src, count):
        us, pushed = [], {}
        for p in range(nb):
            b = block(f, p)
            r = dot(inv[f, b, 0:full_rows], src(b))
            pushed[b] = r[:bs]
            us.append(r[low:])
        return us, pushed

    def solve(f, wv, pushed, dst, s=None):
        for p in range(nb):
            b = block(f, p)
            dst[b] = pushed[b] if s is None else pushed[b] - coupled(f, b, s)
            s = part(wv, p) if s is None else s + part(wv, p)

    def columns(x):
        hi = x.astype(bf16)
        l = rows_lanes(bs)
        rest = x - hi.astype(f32)
        low = jnp.where(between(bs, lo_at, v_end), x + pltpu.roll(rest, n, 1), x)
        return low.astype(bf16)

    for cp in small[:4] + large[0]:
        cp.wait()
    tall_l = reduce_left(0)
    qs_l, us_l = lead(0)
    z_l = {}
    for _ in couple(0, z_l, nb):
        pass
    for cp in small[4:] + large[1]:
        cp.wait()
    tall_u = reduce_left(1)
    qs_u, us_u = lead(1)
    out_l, out_u = [], []
    together(
        invert_steps(qs_l, w, out_l), invert_steps(qs_u, w, out_u), couple(1, {}, -(-nb // 3))
    )
    wp[0] = joined(out_l).astype(bf16)
    wp[1] = joined(out_u).astype(bf16)
    w_a = advance(0, us_l)
    w_u = advance(1, us_u)
    base_u = jnp.concatenate(tall_u, axis=0)
    base_l = jnp.concatenate(tall_l, axis=0)
    adjoint = base_u + dot(diagonal(tops(out_u)), base_u.astype(bf16))

    s = eye_l
    turn = {}
    for p in range(nb):
        y[p] = jnp.where(between(bs, v_at, v_end), z_l[p], 0.0) - coupled(0, p, s)
        s = s + part(w_a, p)

    rows_a = [part(adjoint, block(1, b)).astype(bf16) for b in range(nb)]
    for b in range(nb):
        turn[b] = dot(rows_a[b], cm[0, b])
    later = {nb - 1: None}
    for b in range(nb - 1, 0, -1):
        later[b - 1] = turn[b] if later[b] is None else later[b] + turn[b]
    wide_y = None
    for b in range(nb - 1):
        full = jnp.concatenate([out_l[b][t] + home(b, t) for t in range(nb // per)], axis=1)
        t = dot(later[b].astype(bf16)[:, :w], full.astype(bf16))
        wide_y = t if wide_y is None else wide_y + t
    y_tiles = [wide_y[:, t * LANES : (t + 1) * LANES] for t in range(nb // per)]
    base_hi = base_l.astype(bf16)
    near_rows = base_l + dot(diagonal(tops(out_l)), base_hi)
    far_rows = dot(diagonal(y_tiles), base_hi)
    for b in range(nb):
        adj[b, :w] = part(near_rows, b).astype(bf16)
        adj[b, w:] = (dot(rows_a[b], inv[0, b, 0:bs]) - part(far_rows, b)).astype(bf16)

    def twin(b):
        x = y[b]
        hi = x.astype(bf16)
        return jnp.where(between(bs, lo_at, v_end), x - hi.astype(f32), x).astype(bf16)

    us, pushed = push(1, twin, nb)
    w_b = advance(1, us)
    end_a, end_u, end_b = total(w_a, nb), total(w_u, nb), total(w_b, nb)
    shift = pltpu.roll(end_b, n, 1)
    tile0 = jnp.where(lane < w, end_a, end_u)
    tile0 = jnp.where(between(w, v_at, lo_at), end_a, tile0)
    tile0 = jnp.where(between(w, lo_at, v_end), end_b + shift, tile0)
    tile0 = jnp.where(lane >= v_end, pltpu.roll(end_b, v_end, 1), tile0)
    send0[...] = tile0.astype(bf16)

    def peer_of(i):
        return i + (i + R - me) // R

    def copy(k, src, dst, i):
        return pltpu.make_async_remote_copy(
            src_ref=src, dst_ref=dst.at[me], send_sem=send_sem.at[k, i],
            recv_sem=recv_sem.at[k, me], device_id={"rows": peer_of(i)}, device_id_type=MESH,
        )

    def arrive(k, src, dst, i):
        peer = peer_of(i)
        pltpu.make_async_remote_copy(
            src_ref=src, dst_ref=dst.at[peer], send_sem=send_sem.at[k, i],
            recv_sem=recv_sem.at[k, peer], device_id={"rows": peer}, device_id_type=MESH,
        ).wait_recv()

    pl.semaphore_wait(barrier, R - 1)
    each(R - 1, lambda i: copy(0, send0, got0, i).start())
    got0[me] = send0[...]

    solve(1, w_b + w_u, pushed, x1, eye_u)
    ends = None
    for b in range(nb):
        r = dot(adj[b], x1[b].astype(bf16))
        ends = r if ends is None else ends + r
    send1[...] = ends.astype(bf16)
    each(R - 1, lambda i: copy(1, send1, got1, i).start())
    got1[me] = send1[...]

    @pl.when(me >= 0)
    def _():
        def flip(dst):
            def src(b, x):
                cols = columns(x)
                dst[b] = cols.T
                return cols

            return src

        keep = flip(t1)
        us, pushed = push(0, lambda b: keep(b, x1[b]), nb)
        solve(0, advance(0, us), pushed, y)
        us, pushed = push(1, lambda b: columns(y[b]), nb)
        solve(1, advance(1, us), pushed, x2)
        keep = flip(t2)
        for b in range(nb):
            keep(b, x2[b])

    spot = jnp.where((lane == row + v_at) & (row < n), 1.0, 0.0)[:n]

    def near(a, b, own):
        a, b = (zero if a is None else a), (zero if b is None else b)
        v = spot if own else gap
        return jnp.concatenate([a, b, v, v, zero], axis=0)

    def late(b, own, a=None):
        return jnp.concatenate(
            [zero, zero if a is None else a, gap, spot if own else gap, b], axis=0
        )

    def times(tile, x):
        hi, lo = split(x)
        return dot(tile, hi) + dot(tile, lo)

    def tall(x):
        return jnp.concatenate(split(x), axis=0)

    def halves(r):
        return r[:n] + r[n:]

    def across(x):
        return x.T[v_at:lo_at]

    mine = pl.ds(pl.multiple_of(me * w, w), w)

    def opening(dst, src):
        one = tall(across(near(states[0, mine], states[1, mine], True)))
        for b in range(nb):
            dst[:, b * bs : (b + 1) * bs] = halves(dot(one, src[b]))

    def closing(last):
        two = tall(last)
        for b in range(nb):
            at = slice(b * bs, (b + 1) * bs)
            second[:, at] = second[:, at] + halves(dot(two, t1[b]))

    each(R - 1, lambda i: arrive(0, send0, got0, i))
    if R <= 8:
        up, down = list(range(R)), list(range(R - 1, -1, -1))
        tiles = [got0[d] for d in range(R)]
        wide = [t.astype(f32) for t in tiles]
        inner = lane < w
        out_f, out_b = [], []
        together(
            invert_steps([jnp.where(inner, -wide[d], 0.0) for d in up], w, out_f),
            invert_steps(
                [jnp.where(inner, -pltpu.roll(wide[d], LANES - w, 1), 0.0) for d in down], w, out_b
            ),
        )
        tiled = range(R // per)

        def carry(m, out, order):
            u = jnp.concatenate([m[d] for d in order], axis=0)
            wv = u + dot(joined(out).astype(bf16), u.astype(bf16))
            s, res = zero, [None] * R
            for i, d in enumerate(order):
                res[d] = s
                s = s + part(wv, i)
            return res

        mid = between(w, v_at, lo_at)
        s1 = carry([jnp.where(mid, wide[d], 0.0) for d in up], out_f, up)
        m2 = [dot(tiles[d], late(s1[d], True).astype(bf16)) for d in up]
        s2 = carry(m2, out_b, down)
        for d in up:
            states[0, d * w : (d + 1) * w] = s1[d]
            states[1, d * w : (d + 1) * w] = s2[d]
        g = [across(near(s1[d], s2[d], True)).astype(bf16) for d in up]

        def reach(k, out, order):
            s = [zero for _ in tiled]
            for i, d in enumerate(order):
                for t in tiled:
                    maps[k, d * w : (d + 1) * w, t * LANES : (t + 1) * LANES] = s[t]
                s = [s[t] + out[i][t] + home(i, t) for t in tiled]
            return maps[k, mine]

        own_f = reach(0, out_f, up)
        own_b = reach(1, out_b, down)
        whole_f = maps[0].astype(bf16)
        gates = []
        own_bt = own_b.T
        for d in up:
            i = R - 1 - d
            gates.append(own_bt[i * w : (i + 1) * w])
        across_rows = jnp.concatenate(
            [
                lax.dot_general(
                    pltpu.roll(wide[d], w, 1).astype(bf16)[:, :w], gates[d].astype(bf16),
                    (((0,), (0,)), ((), ())), preferred_element_type=f32,
                )
                for d in up
            ],
            axis=0,
        )
        joint_t = lax.dot_general(
            whole_f, across_rows.astype(bf16), (((0,), (0,)), ((), ())), preferred_element_type=f32
        )
        own_ft = own_f.T
        none = jnp.zeros((w, w), f32)
        moves = []
        for d in up:
            at_d = slice(d * w, (d + 1) * w)
            moves.append(
                jnp.concatenate(
                    [
                        jnp.concatenate([own_ft[at_d], joint_t[at_d], none, none], axis=1),
                        jnp.concatenate([none, gates[d], none, none], axis=1),
                    ],
                    axis=0,
                ).astype(bf16)
            )
        opening(first, t1)
        each(R - 1, lambda i: arrive(1, send1, got1, i))
        heard = [dot_nt(g[d], got1[d]).astype(bf16) for d in up]
        opening(second, t2)
        last = None
        for d in up:
            r = dot(heard[d], moves[d])
            last = r if last is None else last + r
        closing(last)
    else:
        def at(d):
            return pl.ds(pl.multiple_of(d * w, w), w)

        def walk(k, step, back):
            def body(i, s):
                d = R - 1 - i if back else i
                states[k, at(d)] = s
                return s + step(d, s)

            lax.fori_loop(0, R, body, zero)

        def joint(d):
            return near(states[0, at(d)], states[1, at(d)], True)

        def ahead(s, own):
            v = spot if own else gap
            return jnp.concatenate([s, zero, v, gap, zero], axis=0)

        walk(0, lambda d, s: times(got0[d], ahead(s, True)), False)
        walk(1, lambda d, s: times(got0[d], late(states[0, at(d)], True, s)), True)
        opening(first, t1)
        opening(second, t2)
        each(R - 1, lambda i: arrive(1, send1, got1, i))
        walk(
            2,
            lambda d, s: times(got1[d, :w], joint(d)) + times(got0[d], ahead(s, False)),
            False,
        )
        walk(
            3,
            lambda d, s: times(got1[d, w:], joint(d))
            + times(got0[d], late(states[2, at(d)], False, s)),
            True,
        )
        closing(across(near(states[2, mine], states[3, mine], False)))

    each(R - 1, lambda i: copy(0, send0, got0, i).wait_send())
    each(R - 1, lambda i: copy(1, send1, got1, i).wait_send())


def deliver(x, y, x_out, y_out, sem):
    copies = [
        pltpu.make_async_copy(src, dst, sem.at[i])
        for i, (src, dst) in enumerate(((x, x_out), (y, y_out)))
    ]
    for cp in copies:
        cp.start()
    for cp in copies:
        cp.wait()


def local(R, rhs, linv, lleft, lright, uinv, uleft, uright, ranks):
    nb, bs, w = lleft.shape
    n = rhs.shape[0]
    flip = lambda a: jnp.swapaxes(a, 1, 2)
    vmem = pl.BlockSpec(memory_space=pltpu.VMEM)
    hbm = pl.BlockSpec(memory_space=pltpu.HBM)
    out = jax.ShapeDtypeStruct(rhs.shape, f32)
    slim = pltpu.VMEM((nb, w, bs), bf16)
    tall = pltpu.VMEM((nb, bs, LANES), f32)
    args = (rhs, linv, flip(lleft), flip(lright), uinv, flip(uleft), flip(uright), ranks)
    results = pl.pallas_call(
        functools.partial(kernel, R, nb, bs, w, n),
        out_shape=(out, out),
        in_specs=[hbm] * 8,
        out_specs=(vmem, vmem),
        scratch_shapes=[
            pltpu.VMEM(rhs.shape, bf16),
            slim, slim, slim, slim,
            pltpu.SMEM(ranks.shape, jnp.int32),
            pltpu.VMEM((2, nb, bs + w, bs), bf16),
            pltpu.VMEM((nb, 2 * w, bs), bf16),
            pltpu.VMEM((2, nb, bs, LANES), bf16),
            pltpu.VMEM((2, nb * w, nb * w), bf16),
            tall, tall, tall,
            pltpu.VMEM((nb, LANES, bs), bf16),
            pltpu.VMEM((nb, LANES, bs), bf16),
            pltpu.VMEM((w, LANES), bf16),
            pltpu.VMEM((2 * w, LANES), bf16),
            pltpu.VMEM((R, w, LANES), bf16),
            pltpu.VMEM((R, 2 * w, LANES), bf16),
            pltpu.VMEM((4, R * w, LANES), f32),
            pltpu.VMEM((2, R * w, min(R, 8) * w), f32),
            pltpu.SemaphoreType.DMA((6,)),
            pltpu.SemaphoreType.DMA((2, nb)),
            pltpu.SemaphoreType.DMA((2, R)),
            pltpu.SemaphoreType.DMA((2, R)),
        ],
        compiler_params=pltpu.CompilerParams(
            collective_id=0, has_side_effects=True, vmem_limit_bytes=33554432
        ),
    )(*[pltpu.with_memory_space_constraint(a, pltpu.HBM) for a in args])
    return pl.pallas_call(
        deliver,
        out_shape=(out, out),
        in_specs=[pl.BlockSpec(memory_space=pl.ANY)] * 2,
        out_specs=(hbm, hbm),
        scratch_shapes=[pltpu.SemaphoreType.DMA((2,))],
        compiler_params=pltpu.CompilerParams(vmem_limit_bytes=1048576),
    )(*[pltpu.with_memory_space_constraint(r, pltpu.VMEM) for r in results])


def solution(mesh):
    blocks = P("rows", None, None)
    placed = (P("rhs", "rows"),) + (blocks,) * 6 + (P(None, "rows"),)
    return jax.shard_map(
        functools.partial(local, mesh.shape["rows"]),
        mesh=mesh,
        in_specs=placed,
        out_specs=(P("rhs", "rows"), P("rhs", "rows")),
        check_vma=False,
    )
```

```python
import functools

import jax
import jax.numpy as jnp
from jax import lax
from jax.experimental import pallas as pl
from jax.experimental.pallas import tpu as pltpu
from jax.sharding import PartitionSpec as P

MESH = pl.DeviceIdType.MESH
LANES = 128
f32, bf16 = jnp.float32, jnp.bfloat16


def split(x):
    hi = x.astype(bf16)
    return hi, (x - hi.astype(f32)).astype(bf16)


def dot(a, b):
    return jnp.dot(a, b, preferred_element_type=f32)


def dot_nt(a, b):
    return lax.dot_general(a, b, (((1,), (1,)), ((), ())), preferred_element_type=f32)


def each(count, body):
    if count <= 8:
        for i in range(count):
            body(i)
    else:
        lax.fori_loop(0, count, lambda i, c: (body(i), c)[1], 0)


def rows_lanes(rows):
    return lax.broadcasted_iota(jnp.int32, (rows, LANES), 1)


def invert_steps(qs, w, out):
    count = len(qs)
    lane = rows_lanes(w)
    row = lax.broadcasted_iota(jnp.int32, (w, LANES), 0)
    per = LANES // w
    tiles = count // per
    zero = jnp.zeros((w, LANES), f32)
    out.extend([zero] * tiles for _ in range(count))
    groups = []
    for b in range(count):
        home = jnp.where(lane == row + (b % per) * w, 1.0, 0.0)
        groups.append(([b], [qs[b]], -qs[b], {b // per: home}))
    while len(groups) > 1:
        merged = []
        last = len(groups) == 2
        for (ia, ra, da, ga), (ib, rb, db, gb) in zip(groups[::2], groups[1::2]):
            lhs = jnp.concatenate(rb if last else [*rb, db], axis=0).astype(bf16)[:, :w]
            tags = sorted(ga)
            rhs = jnp.concatenate([ga[t] for t in tags] + ([] if last else [da]), axis=1).astype(bf16)
            res = dot(lhs, rhs)
            at = len(tags) * LANES
            for i, b in enumerate(ib):
                for j, t in enumerate(tags):
                    out[b][t] = out[b][t] - res[w * i : w * (i + 1), LANES * j : LANES * (j + 1)]
            if last:
                continue
            tail = w * len(ib)
            moved = [rb[i] + res[w * i : w * (i + 1), at:] for i in range(len(ib))]
            g = {t: ga[t] + res[tail:, LANES * j : LANES * (j + 1)] for j, t in enumerate(tags)}
            for t in gb:
                g[t] = g[t] + gb[t] if t in g else gb[t]
            merged.append((ia + ib, ra + moved, da + db + res[tail:, at:], g))
        groups = merged
        yield
        if last:
            break


def together(*steps):
    live = list(steps)
    while live:
        live = [s for s in live if next(s, s) is not s]


def joined(out):
    return jnp.concatenate([jnp.concatenate(parts, axis=1) for parts in out], axis=0)


def kernel(
    R, nb, bs, w, n,
    rhs_h, linv_h, llt_h, lrt_h, uinv_h, ult_h, urt_h, ranks_h,
    first, second,
    rhs, llt, lrt, ult, urt, ranks,
    inv, adj, cm, wp, y, x1, x2, t1, t2, send0, send1, got0, got1, states, maps,
    load_sem, block_sem, send_sem, recv_sem,
):
    me = lax.axis_index("rows")
    small = [
        pltpu.make_async_copy(src, dst, load_sem.at[i])
        for i, (src, dst) in enumerate(
            ((lrt_h, lrt), (ranks_h, ranks), (llt_h, llt), (rhs_h, rhs), (urt_h, urt), (ult_h, ult))
        )
    ]
    large = [
        [
            pltpu.make_async_copy(src.at[b], inv.at[f, b, 0:bs], block_sem.at[f, b])
            for b in range(nb)
        ]
        for f, src in ((0, linv_h), (1, uinv_h))
    ]
    for cp in small[:4] + large[0] + small[4:] + large[1]:
        cp.start()

    barrier = pltpu.get_barrier_semaphore()

    def greet(i):
        pl.semaphore_signal(
            barrier, inc=1, device_id={"rows": lax.rem(me + i + 1, R)}, device_id_type=MESH
        )

    each(R - 1, greet)

    lane = rows_lanes(w)
    row = lax.broadcasted_iota(jnp.int32, (w, LANES), 0)
    v_at, lo_at, v_end = 2 * w, 2 * w + n, 2 * w + 2 * n
    zero = jnp.zeros((w, LANES), f32)
    gap = jnp.zeros((n, LANES), f32)
    eye_l = jnp.where(lane == row, 1.0, 0.0)
    eye_u = jnp.where(lane == row + w, 1.0, 0.0)
    low, full_rows = bs, bs + w

    def block(f, p):
        return p if f == 0 else nb - 1 - p

    def between(rows, lo, hi):
        l = rows_lanes(rows)
        return (l >= lo) & (l < hi)

    def part(x, p):
        return x[p * w : (p + 1) * w]

    lefts, rights = (llt, ult), (lrt, urt)

    def reduce_left(f):
        wide_row = lax.broadcasted_iota(jnp.int32, (w, bs), 0)
        tall = []
        for p in range(nb):
            b = block(f, p)
            mt = jnp.where(wide_row < ranks[f, b], rights[f][b].astype(f32), 0.0).astype(bf16)
            t = dot(mt, inv[f, b, 0:bs])
            inv[f, b, low:full_rows] = t.astype(bf16)
            tall.append(t)
        return tall

    def lead(f):
        qs, us = [], []
        for p in range(nb):
            b = block(f, p)
            cols = lefts[f][b]
            if f == 0:
                cols = jnp.concatenate([cols, rhs[:, b * bs : (b + 1) * bs]], axis=0)
            r = dot_nt(inv[f, b, low:full_rows], cols)
            r = jnp.concatenate([r, jnp.zeros((w, LANES - r.shape[1]), f32)], axis=1)
            qs.append(jnp.where(lane < w, r, 0.0))
            if f == 0:
                u = jnp.where(lane < w, -r, 0.0)
                u = jnp.where(between(w, v_at, lo_at), pltpu.roll(r, v_at - w, 1), u)
                us.append(jnp.where(between(w, lo_at, v_end), pltpu.roll(r, lo_at - w, 1), u))
            else:
                us.append(jnp.where(between(w, w, v_at), pltpu.roll(-r, w, 1), 0.0))
        return qs, us

    def couple(f, pushed, chunk):
        for p in range(nb):
            b = block(f, p)
            left = lefts[f][b]
            cols = [left, left]
            if f == 0:
                v = rhs[:, b * bs : (b + 1) * bs]
                cols += [v, v]
            z = dot_nt(inv[f, b, 0:bs], jnp.concatenate(cols, axis=0))
            z = jnp.concatenate([z, jnp.zeros((bs, LANES - z.shape[1]), f32)], axis=1)
            cm[f, b] = z.astype(bf16)
            pushed[b] = z
            if p % chunk == chunk - 1:
                yield

    per = LANES // w

    def diagonal(tiles):
        return jnp.concatenate(
            [
                jnp.concatenate(
                    [
                        jnp.where(lane // w == p % per, tiles[t], 0.0) if t == p // per else zero
                        for t in range(len(tiles))
                    ],
                    axis=1,
                )
                for p in range(len(tiles) * per)
            ],
            axis=0,
        ).astype(bf16)

    def tops(out):
        return [sum(out[p][t] for p in range(1, len(out))) for t in range(len(out[0]))]

    def home(p, t):
        return jnp.where(lane == row + p % per * w, 1.0, 0.0) if t == p // per else zero

    def advance(f, us):
        u = jnp.concatenate(us, axis=0)
        return u + dot(wp[f], u.astype(bf16))

    def total(x, count):
        s = part(x, 0)
        for p in range(1, count):
            s = s + part(x, p)
        return s

    def coupled(f, b, s):
        return dot(cm[f, b][:, : 2 * w], jnp.concatenate(split(s), axis=0))

    def push(f, src, count):
        us, pushed = [], {}
        for p in range(nb):
            b = block(f, p)
            r = dot(inv[f, b, 0:full_rows], src(b))
            pushed[b] = r[:bs]
            us.append(r[low:])
        return us, pushed

    def solve(f, wv, pushed, dst, s=None):
        for p in range(nb):
            b = block(f, p)
            dst[b] = pushed[b] if s is None else pushed[b] - coupled(f, b, s)
            s = part(wv, p) if s is None else s + part(wv, p)

    def columns(x):
        hi = x.astype(bf16)
        l = rows_lanes(bs)
        rest = x - hi.astype(f32)
        low = jnp.where(between(bs, lo_at, v_end), x + pltpu.roll(rest, n, 1), x)
        return low.astype(bf16)

    for cp in small[:4] + large[0]:
        cp.wait()
    tall_l = reduce_left(0)
    qs_l, us_l = lead(0)
    z_l = {}
    for _ in couple(0, z_l, nb):
        pass
    for cp in small[4:] + large[1]:
        cp.wait()
    tall_u = reduce_left(1)
    qs_u, us_u = lead(1)
    out_l, out_u = [], []
    together(
        invert_steps(qs_l, w, out_l), invert_steps(qs_u, w, out_u), couple(1, {}, -(-nb // 3))
    )
    wp[0] = joined(out_l).astype(bf16)
    wp[1] = joined(out_u).astype(bf16)
    w_a = advance(0, us_l)
    w_u = advance(1, us_u)
    base_u = jnp.concatenate(tall_u, axis=0)
    base_l = jnp.concatenate(tall_l, axis=0)
    adjoint = base_u + dot(diagonal(tops(out_u)), base_u.astype(bf16))

    s = eye_l
    turn = {}
    for p in range(nb):
        y[p] = jnp.where(between(bs, v_at, v_end), z_l[p], 0.0) - coupled(0, p, s)
        s = s + part(w_a, p)

    rows_a = [part(adjoint, block(1, b)).astype(bf16) for b in range(nb)]
    for b in range(nb):
        turn[b] = dot(rows_a[b], cm[0, b])
    later = {nb - 1: None}
    for b in range(nb - 1, 0, -1):
        later[b - 1] = turn[b] if later[b] is None else later[b] + turn[b]
    wide_y = None
    for b in range(nb - 1):
        full = jnp.concatenate([out_l[b][t] + home(b, t) for t in range(nb // per)], axis=1)
        t = dot(later[b].astype(bf16)[:, :w], full.astype(bf16))
        wide_y = t if wide_y is None else wide_y + t
    y_tiles = [wide_y[:, t * LANES : (t + 1) * LANES] for t in range(nb // per)]
    base_hi = base_l.astype(bf16)
    near_rows = base_l + dot(diagonal(tops(out_l)), base_hi)
    far_rows = dot(diagonal(y_tiles), base_hi)
    for b in range(nb):
        adj[b, :w] = part(near_rows, b).astype(bf16)
        adj[b, w:] = (dot(rows_a[b], inv[0, b, 0:bs]) - part(far_rows, b)).astype(bf16)

    def twin(b):
        x = y[b]
        hi = x.astype(bf16)
        return jnp.where(between(bs, lo_at, v_end), x - hi.astype(f32), x).astype(bf16)

    us, pushed = push(1, twin, nb)
    w_b = advance(1, us)
    end_a, end_u, end_b = total(w_a, nb), total(w_u, nb), total(w_b, nb)
    shift = pltpu.roll(end_b, n, 1)
    tile0 = jnp.where(lane < w, end_a, end_u)
    tile0 = jnp.where(between(w, v_at, lo_at), end_a, tile0)
    tile0 = jnp.where(between(w, lo_at, v_end), end_b + shift, tile0)
    tile0 = jnp.where(lane >= v_end, pltpu.roll(end_b, v_end, 1), tile0)
    send0[...] = tile0.astype(bf16)

    def peer_of(i):
        return i + (i + R - me) // R

    def copy(k, src, dst, i):
        return pltpu.make_async_remote_copy(
            src_ref=src, dst_ref=dst.at[me], send_sem=send_sem.at[k, i],
            recv_sem=recv_sem.at[k, me], device_id={"rows": peer_of(i)}, device_id_type=MESH,
        )

    def arrive(k, src, dst, i):
        peer = peer_of(i)
        pltpu.make_async_remote_copy(
            src_ref=src, dst_ref=dst.at[peer], send_sem=send_sem.at[k, i],
            recv_sem=recv_sem.at[k, peer], device_id={"rows": peer}, device_id_type=MESH,
        ).wait_recv()

    pl.semaphore_wait(barrier, R - 1)
    near_count = max(1, R // 4)
    each(near_count, lambda i: copy(0, send0, got0, i).start())
    got0[me] = send0[...]

    solve(1, w_b + w_u, pushed, x1, eye_u)
    ends = None
    for b in range(nb):
        r = dot(adj[b], x1[b].astype(bf16))
        ends = r if ends is None else ends + r
    send1[...] = ends.astype(bf16)
    each(near_count, lambda i: copy(1, send1, got1, i).start())
    each(R - 1 - near_count, lambda i: copy(0, send0, got0, near_count + i).start())
    each(R - 1 - near_count, lambda i: copy(1, send1, got1, near_count + i).start())
    got1[me] = send1[...]

    @pl.when(me >= 0)
    def _():
        def flip(dst):
            def src(b, x):
                cols = columns(x)
                dst[b] = cols.T
                return cols

            return src

        keep = flip(t1)
        us, pushed = push(0, lambda b: keep(b, x1[b]), nb)
        solve(0, advance(0, us), pushed, y)
        us, pushed = push(1, lambda b: columns(y[b]), nb)
        solve(1, advance(1, us), pushed, x2)
        keep = flip(t2)
        for b in range(nb):
            keep(b, x2[b])

    spot = jnp.where((lane == row + v_at) & (row < n), 1.0, 0.0)[:n]

    def near(a, b, own):
        a, b = (zero if a is None else a), (zero if b is None else b)
        v = spot if own else gap
        return jnp.concatenate([a, b, v, v, zero], axis=0)

    def late(b, own, a=None):
        return jnp.concatenate(
            [zero, zero if a is None else a, gap, spot if own else gap, b], axis=0
        )

    def times(tile, x):
        hi, lo = split(x)
        return dot(tile, hi) + dot(tile, lo)

    def tall(x):
        return jnp.concatenate(split(x), axis=0)

    def halves(r):
        return r[:n] + r[n:]

    def across(x):
        return x.T[v_at:lo_at]

    mine = pl.ds(pl.multiple_of(me * w, w), w)

    def opening(dst, src):
        one = tall(across(near(states[0, mine], states[1, mine], True)))
        for b in range(nb):
            dst[:, b * bs : (b + 1) * bs] = halves(dot(one, src[b]))

    def closing(last):
        two = tall(last)
        for b in range(nb):
            at = slice(b * bs, (b + 1) * bs)
            second[:, at] = second[:, at] + halves(dot(two, t1[b]))

    each(R - 1, lambda i: arrive(0, send0, got0, i))
    if R <= 8:
        up, down = list(range(R)), list(range(R - 1, -1, -1))
        tiles = [got0[d] for d in range(R)]
        wide = [t.astype(f32) for t in tiles]
        inner = lane < w
        out_f, out_b = [], []
        together(
            invert_steps([jnp.where(inner, -wide[d], 0.0) for d in up], w, out_f),
            invert_steps(
                [jnp.where(inner, -pltpu.roll(wide[d], LANES - w, 1), 0.0) for d in down], w, out_b
            ),
        )
        tiled = range(R // per)

        def carry(m, out, order):
            u = jnp.concatenate([m[d] for d in order], axis=0)
            wv = u + dot(joined(out).astype(bf16), u.astype(bf16))
            s, res = zero, [None] * R
            for i, d in enumerate(order):
                res[d] = s
                s = s + part(wv, i)
            return res

        mid = between(w, v_at, lo_at)
        s1 = carry([jnp.where(mid, wide[d], 0.0) for d in up], out_f, up)
        m2 = [dot(tiles[d], late(s1[d], True).astype(bf16)) for d in up]
        s2 = carry(m2, out_b, down)
        for d in up:
            states[0, d * w : (d + 1) * w] = s1[d]
            states[1, d * w : (d + 1) * w] = s2[d]
        g = [across(near(s1[d], s2[d], True)).astype(bf16) for d in up]

        def reach(k, out, order):
            s = [zero for _ in tiled]
            for i, d in enumerate(order):
                for t in tiled:
                    maps[k, d * w : (d + 1) * w, t * LANES : (t + 1) * LANES] = s[t]
                s = [s[t] + out[i][t] + home(i, t) for t in tiled]
            return maps[k, mine]

        own_f = reach(0, out_f, up)
        own_b = reach(1, out_b, down)
        whole_f = maps[0].astype(bf16)
        gates = []
        own_bt = own_b.T
        for d in up:
            i = R - 1 - d
            gates.append(own_bt[i * w : (i + 1) * w])
        across_rows = jnp.concatenate(
            [
                lax.dot_general(
                    pltpu.roll(wide[d], w, 1).astype(bf16)[:, :w], gates[d].astype(bf16),
                    (((0,), (0,)), ((), ())), preferred_element_type=f32,
                )
                for d in up
            ],
            axis=0,
        )
        joint_t = lax.dot_general(
            whole_f, across_rows.astype(bf16), (((0,), (0,)), ((), ())), preferred_element_type=f32
        )
        own_ft = own_f.T
        none = jnp.zeros((w, w), f32)
        moves = []
        for d in up:
            at_d = slice(d * w, (d + 1) * w)
            moves.append(
                jnp.concatenate(
                    [
                        jnp.concatenate([own_ft[at_d], joint_t[at_d], none, none], axis=1),
                        jnp.concatenate([none, gates[d], none, none], axis=1),
                    ],
                    axis=0,
                ).astype(bf16)
            )
        opening(first, t1)
        each(R - 1, lambda i: arrive(1, send1, got1, i))
        heard = [dot_nt(g[d], got1[d]).astype(bf16) for d in up]
        opening(second, t2)
        last = None
        for d in up:
            r = dot(heard[d], moves[d])
            last = r if last is None else last + r
        closing(last)
    else:
        def at(d):
            return pl.ds(pl.multiple_of(d * w, w), w)

        def walk(k, step, back):
            def body(i, s):
                d = R - 1 - i if back else i
                states[k, at(d)] = s
                return s + step(d, s)

            lax.fori_loop(0, R, body, zero)

        def joint(d):
            return near(states[0, at(d)], states[1, at(d)], True)

        def ahead(s, own):
            v = spot if own else gap
            return jnp.concatenate([s, zero, v, gap, zero], axis=0)

        walk(0, lambda d, s: times(got0[d], ahead(s, True)), False)
        walk(1, lambda d, s: times(got0[d], late(states[0, at(d)], True, s)), True)
        opening(first, t1)
        opening(second, t2)
        each(R - 1, lambda i: arrive(1, send1, got1, i))
        walk(
            2,
            lambda d, s: times(got1[d, :w], joint(d)) + times(got0[d], ahead(s, False)),
            False,
        )
        walk(
            3,
            lambda d, s: times(got1[d, w:], joint(d))
            + times(got0[d], late(states[2, at(d)], False, s)),
            True,
        )
        closing(across(near(states[2, mine], states[3, mine], False)))

    each(R - 1, lambda i: copy(0, send0, got0, i).wait_send())
    each(R - 1, lambda i: copy(1, send1, got1, i).wait_send())


def deliver(x, y, x_out, y_out, sem):
    copies = [
        pltpu.make_async_copy(src, dst, sem.at[i])
        for i, (src, dst) in enumerate(((x, x_out), (y, y_out)))
    ]
    for cp in copies:
        cp.start()
    for cp in copies:
        cp.wait()


def local(R, rhs, linv, lleft, lright, uinv, uleft, uright, ranks):
    nb, bs, w = lleft.shape
    n = rhs.shape[0]
    flip = lambda a: jnp.swapaxes(a, 1, 2)
    vmem = pl.BlockSpec(memory_space=pltpu.VMEM)
    hbm = pl.BlockSpec(memory_space=pltpu.HBM)
    out = jax.ShapeDtypeStruct(rhs.shape, f32)
    slim = pltpu.VMEM((nb, w, bs), bf16)
    tall = pltpu.VMEM((nb, bs, LANES), f32)
    args = (rhs, linv, flip(lleft), flip(lright), uinv, flip(uleft), flip(uright), ranks)
    results = pl.pallas_call(
        functools.partial(kernel, R, nb, bs, w, n),
        out_shape=(out, out),
        in_specs=[hbm] * 8,
        out_specs=(vmem, vmem),
        scratch_shapes=[
            pltpu.VMEM(rhs.shape, bf16),
            slim, slim, slim, slim,
            pltpu.SMEM(ranks.shape, jnp.int32),
            pltpu.VMEM((2, nb, bs + w, bs), bf16),
            pltpu.VMEM((nb, 2 * w, bs), bf16),
            pltpu.VMEM((2, nb, bs, LANES), bf16),
            pltpu.VMEM((2, nb * w, nb * w), bf16),
            tall, tall, tall,
            pltpu.VMEM((nb, LANES, bs), bf16),
            pltpu.VMEM((nb, LANES, bs), bf16),
            pltpu.VMEM((w, LANES), bf16),
            pltpu.VMEM((2 * w, LANES), bf16),
            pltpu.VMEM((R, w, LANES), bf16),
            pltpu.VMEM((R, 2 * w, LANES), bf16),
            pltpu.VMEM((4, R * w, LANES), f32),
            pltpu.VMEM((2, R * w, min(R, 8) * w), f32),
            pltpu.SemaphoreType.DMA((6,)),
            pltpu.SemaphoreType.DMA((2, nb)),
            pltpu.SemaphoreType.DMA((2, R)),
            pltpu.SemaphoreType.DMA((2, R)),
        ],
        compiler_params=pltpu.CompilerParams(
            collective_id=0, has_side_effects=True, vmem_limit_bytes=33554432
        ),
    )(*[pltpu.with_memory_space_constraint(a, pltpu.HBM) for a in args])
    return pl.pallas_call(
        deliver,
        out_shape=(out, out),
        in_specs=[pl.BlockSpec(memory_space=pl.ANY)] * 2,
        out_specs=(hbm, hbm),
        scratch_shapes=[pltpu.SemaphoreType.DMA((2,))],
        compiler_params=pltpu.CompilerParams(vmem_limit_bytes=1048576),
    )(*[pltpu.with_memory_space_constraint(r, pltpu.VMEM) for r in results])


def solution(mesh):
    blocks = P("rows", None, None)
    placed = (P("rhs", "rows"),) + (blocks,) * 6 + (P(None, "rows"),)
    return jax.shard_map(
        functools.partial(local, mesh.shape["rows"]),
        mesh=mesh,
        in_specs=placed,
        out_specs=(P("rhs", "rows"), P("rhs", "rows")),
        check_vma=False,
    )
```
